32 devices in a mesh: batch: 4 (over y, core), tm: 2 (over x), space: 4 (over z).
Axes of the slice: x: 2, y: 2, z: 4, core: 2. Of those that a mesh axis runs over, the one named last changes fastest.
Arguments:
- clip_tokens: bfloat16 [4, 4, 32, 32, 1024], P('batch', None, 'space', 'tm'), may hold values from -6 to 6
- frame_order: int32 [4, 4], P('batch'), may hold values from 0 to 3, each once within a row
- row_reach: int32 [4, 4], P('batch', 'tm'), may hold values from 1 to 4
- spatial_gain: float32 [1024], replicated, may hold values from 0.1 to 1.9
- spatial_heads: bfloat16 [1024, 3072], replicated, may hold values from -2 to 2
- spatial_merge: bfloat16 [1024, 1024], replicated, may hold values from -0.1875 to 0.1875
- temporal_gain: float32 [1024], replicated, may hold values from 0.1 to 1.9
- temporal_heads: bfloat16 [1024, 3072], replicated, may hold values from -2 to 2
- temporal_merge: bfloat16 [1024, 1024], replicated, may hold values from -0.1875 to 0.1875
- cotangent: bfloat16 [4, 4, 32, 32, 1024], P('batch', 'tm', 'space'), may hold values from -0.059814453 to 0.059814453
Outputs:
- output: bfloat16 [4, 4, 32, 32, 1024], P('batch', 'tm', 'space')
- weight_grad: float32 [1024, 1024], P(('tm', 'space'))
The draws below stay inside these ranges and needn't reach their ends.
Inputs may be any that keep to these rules, and one draw needn't show every extreme that they name: Each row of frame_order names every number from 0 to 3 once.
All inputs are finite; a program needn't handle non-finite values.
Results may differ from the reference program's by a relative error of at most 0.025.
Values may be sent and summed in bfloat16 or wider, within the bound.
A program may use at most 128 MiB of HBM per device.

```python
import jax
import jax.numpy as jnp
from jax import lax

COLS = 32
HALO = 4
D = 1024
HEADS = 16
HEAD_DIM = 64
CLIPS = 4
FRAMES = 4
ROWS = 32


def projection_draw(key):
    key_one, key_two, key_three = jax.random.split(key, 3)
    plain_part = jnp.clip(jax.random.normal(key_one, (D, 3 * D), jnp.float32), -6.0, 6.0) * D ** (-0.5)
    return plain_part.astype(jnp.bfloat16)


def draw_spatial_heads(key, part):
    return projection_draw(jax.random.fold_in(key, 11))


def draw_temporal_heads(key, part):
    return projection_draw(jax.random.fold_in(key, 23))


def with_ends(drawn, own_key, smallest, high):
    index_at = [jax.random.randint(jax.random.fold_in(own_key, axis), (), 0, length) for axis, length in enumerate(drawn.shape)]
    longest = drawn.shape.index(max(drawn.shape))
    beside = index_at[:longest] + [(index_at[longest] + 1) % drawn.shape[longest]] + index_at[longest + 1:]
    return drawn.at[tuple(index_at)].set(smallest).at[tuple(beside)].set(high)


def block_levels(own_key, dims, cuts, low, high):
    factor_of, own = 1.0, jax.random.fold_in(own_key, 6)
    for dim, shards_of in cuts:
        steps = jnp.exp(jax.random.uniform(jax.random.fold_in(own, dim), (shards_of,), jnp.float32, low / len(cuts), high / len(cuts)))
        factor_of = factor_of * jnp.repeat(steps, dims[dim] // shards_of).reshape([-1 if axis == dim else 1 for axis in range(len(dims))])
    return factor_of


def gaussian(stream_key, extent, spread, bound, cuts=(), kind=jnp.bfloat16):
    entries = spread * jax.random.normal(stream_key, extent, jnp.float32)
    if cuts:
        entries = entries * block_levels(stream_key, extent, cuts, -0.22, 0.18)
    return jnp.clip(entries, -bound, bound).astype(kind)


def setup_inputs(seed: int = 0) -> dict:
    seeds = jax.random.split(jax.random.key(seed), 11)
    return {
        "clip_tokens": gaussian(seeds[0], (CLIPS, FRAMES, ROWS, COLS, D), 1.0, 6.0, ((0, 4), (2, 4), (3, 2))),
        "frame_order": jax.vmap(lambda own: jax.random.permutation(own, FRAMES))(jax.random.split(seeds[1], CLIPS)).reshape((CLIPS, FRAMES)).astype(jnp.int32),
        "row_reach": with_ends(jax.random.randint(seeds[2], (CLIPS, FRAMES), 1, HALO + 1), jax.random.fold_in(seeds[2], 1), 1, HALO).astype(jnp.int32),
        "spatial_gain": jnp.clip(1.0 + 0.18 * jax.random.normal(seeds[3], (D,), jnp.float32), 0.1, 1.9),
        "spatial_heads": draw_spatial_heads(jax.random.fold_in(seeds[10], 71), 0),
        "spatial_merge": gaussian(seeds[5], (D, D), D ** -0.5, 0.1875),
        "temporal_gain": jnp.clip(1.0 + 0.18 * jax.random.normal(seeds[6], (D,), jnp.float32), 0.1, 1.9),
        "temporal_heads": draw_temporal_heads(jax.random.fold_in(seeds[10], 71), 0),
        "temporal_merge": gaussian(seeds[8], (D, D), D ** -0.5, 0.1875),
        "cotangent": gaussian(seeds[9], (CLIPS, FRAMES, ROWS, COLS, D), 0.01, 0.059814453, ((0, 4), (1, 2), (2, 4))),
    }


floor_term = 0.5

def normalize(values, gain_vector):
    widened = values.astype(jnp.float32)
    scaled = widened * lax.rsqrt(lax.optimization_barrier(jnp.mean(widened * widened, axis=-1, keepdims=True)) + floor_term)
    return (scaled * gain_vector).astype(jnp.bfloat16)

def softmax_rounded(scores, allowed):
    masked = jnp.where(allowed, scores, -1e+30)
    top_score = lax.optimization_barrier(jnp.max(masked, axis=-1, keepdims=True))
    exponent = jnp.exp(masked - top_score)
    return (exponent / lax.optimization_barrier(jnp.sum(exponent, axis=-1, keepdims=True))).astype(jnp.bfloat16)

def spatial_frame(inputs):
    queries, keys_all, values_all, reach_now = inputs
    token_rows = jnp.arange(ROWS * COLS, dtype=jnp.int32) // COLS
    allowed = jnp.abs(token_rows[:, None] - token_rows[None, :]) <= reach_now
    query_heads = queries.astype(jnp.float32).reshape(-1, HEADS, HEAD_DIM)
    key_heads = keys_all.astype(jnp.float32).reshape(-1, HEADS, HEAD_DIM)
    value_heads = values_all.astype(jnp.float32).reshape(-1, HEADS, HEAD_DIM)
    scores = jnp.einsum('qhd,khd->hqk', query_heads, key_heads) * HEAD_DIM ** (-0.5)
    weights = softmax_rounded(scores, allowed[None])
    context = jnp.einsum('hqk,khd->qhd', weights.astype(jnp.float32), value_heads)
    return context.reshape(-1, D).astype(jnp.bfloat16)

def temporal_clip(queries, keys_all, values_all, order_row):
    query_heads = queries.astype(jnp.float32).reshape(FRAMES, -1, HEADS, HEAD_DIM)
    key_heads = keys_all.astype(jnp.float32).reshape(FRAMES, -1, HEADS, HEAD_DIM)
    value_heads = values_all.astype(jnp.float32).reshape(FRAMES, -1, HEADS, HEAD_DIM)
    scores = jnp.einsum('fthd,gthd->thfg', query_heads, key_heads) * HEAD_DIM ** (-0.5)
    allowed = order_row[None, :] <= order_row[:, None]
    weights = softmax_rounded(scores, allowed[None, None])
    context = jnp.einsum('thfg,gthd->fthd', weights.astype(jnp.float32), value_heads)
    return context.reshape(FRAMES, -1, D).astype(jnp.bfloat16)

def reference(clip_tokens, frame_order, row_reach, spatial_gain, spatial_heads, spatial_merge, temporal_gain, temporal_heads, temporal_merge, cotangent):
    tokens = ROWS * COLS

    def one_clip(running, inputs):
        frames_in, order_row, reach_row, cotangent_clip = inputs
        flat_input = frames_in.reshape(FRAMES, tokens, D)
        normed = normalize(flat_input, spatial_gain)
        projected = jnp.dot(normed, spatial_heads, preferred_element_type=jnp.float32).astype(jnp.bfloat16)
        spatial_context = lax.map(spatial_frame, (projected[..., :D], projected[..., D:2 * D], projected[..., 2 * D:], reach_row))
        middle = (flat_input.astype(jnp.float32) + jnp.dot(spatial_context, spatial_merge, preferred_element_type=jnp.float32)).astype(jnp.bfloat16)
        normed_two = normalize(middle, temporal_gain)
        projected_two = jnp.dot(normed_two, temporal_heads, preferred_element_type=jnp.float32).astype(jnp.bfloat16)
        temporal_context = temporal_clip(projected_two[..., :D], projected_two[..., D:2 * D], projected_two[..., 2 * D:], order_row)
        output_clip = (middle.astype(jnp.float32) + jnp.dot(temporal_context, temporal_merge, preferred_element_type=jnp.float32)).astype(jnp.bfloat16)
        gradient = running + lax.dot_general(temporal_context.reshape(-1, D), cotangent_clip.reshape(-1, D), (((0,), (0,)), ((), ())), preferred_element_type=jnp.float32)
        return (gradient, output_clip.reshape(FRAMES, ROWS, COLS, D))
    zero_grad = jnp.zeros((D, D), jnp.float32)
    weight_grad, output = lax.scan(one_clip, zero_grad, (clip_tokens, frame_order, row_reach, cotangent))
    return (output, weight_grad)
```

```python
import functools

import jax
import jax.numpy as jnp
from jax import lax
from jax.experimental import pallas as pl
from jax.experimental.pallas import tpu as pltpu
from jax.sharding import PartitionSpec as P

HALO = 4
HEADS = 16
HEAD_DIM = 64
LANES = 128
TILE = 512
SCALE = HEAD_DIM ** (-0.5)
FLOOR = 0.5
BF = jnp.bfloat16
F32 = jnp.float32
MESH = pl.DeviceIdType.MESH


def block_kernel(dims, *refs):
    ranks, places, parts, frames, chunks, pc, depth = dims
    (clip, order_ref, reach_ref, gain_one, gain_two, w_one, m_one, w_two, m_two, cot_in,
     out, grad,
     xx, pr, nb, w1, o1, w2, o2, ctx1, mid, mids, qs, ks, vs, ctx2, cot, gather, spread, bias, acc,
     axr, a1, ayr, byr, b1, bxr, zb, zr, gp, gr, outv,
     s_load, s_xs, s_xr, s_zs, s_zr, s_ms, s_mr, s_cs, s_cr, s_gs, s_gr, s_out) = refs
    blk = HALO * pc
    span = blk * ranks
    cols = pc * ranks
    tokens = chunks * span
    rows = chunks * HALO
    keys = ranks * frames
    half = depth // 2
    quarter = half // 2
    t, s, b = lax.axis_index("tm"), lax.axis_index("space"), lax.axis_index("batch")
    core, y = b % 2, b // 2
    ny = parts // 2
    lane_part = quarter // ny
    own_rows = depth // ranks
    piece_rows = own_rows // places

    loads = {}

    def load(name, src, dst):
        copy = pltpu.make_async_copy(src, dst, s_load.at[len(loads)])
        copy.start()
        loads[name] = copy

    def ready(*names):
        for name in names:
            loads[name].wait()

    for f in range(frames):
        load(f"x{f}", clip.at[t * frames + f], xx.at[f, 1:chunks + 1, t])
    for part in range(3):
        load(f"w1{part}", w_one.at[:, part * depth:(part + 1) * depth], w1.at[:, part * depth:(part + 1) * depth])
    load("o1", m_one, o1)
    load("w2", w_two, w2)
    load("o2", m_two, o2)
    load("cot", cot_in.at[:, pl.ds(pl.multiple_of(core * half, half), half)], cot.at[0])

    barrier = pltpu.get_barrier_semaphore()
    for axis, me, count in (("tm", t, ranks), ("space", s, places), ("batch", b, parts)):
        for shift in range(1, count):
            pl.semaphore_signal(barrier, inc=1, device_id={axis: (me + shift) % count}, device_id_type=MESH)
    pl.semaphore_wait(barrier, ranks + places + parts - 3)

    def remote(src, dst, send, recv, axis, to):
        return pltpu.make_async_remote_copy(src, dst, send, recv, device_id={axis: to}, device_id_type=MESH)

    x_copies = {}
    for f in range(frames):
        for j in range(1, ranks):
            to = (t + j) % ranks
            copy = remote(clip.at[to * frames + f], xx.at[f, 1:chunks + 1, t], s_xs.at[f, j - 1], s_xr.at[f, j - 1],
                          "tm", to)
            copy.start()
            x_copies[f, j] = copy

    def halo(f, j, up):
        source = (t - j) % ranks
        slot, dest = (1, chunks + 1) if up else (chunks, 0)
        src = xx.at[f, slot, source]
        if j == 0:
            src = clip.at[t * frames + f, slot - 1]
        return remote(src, xx.at[f, dest, source], s_zs.at[int(up), f, j], s_zr.at[int(up), f, j],
                      "space", (s - 1) if up else (s + 1))

    def send_halo(f, j):
        @pl.when(s > 0)
        def _():
            halo(f, j, True).start()

        @pl.when(s < places - 1)
        def _():
            halo(f, j, False).start()

    def wait_halo(f, j):
        @pl.when(s > 0)
        def _():
            halo(f, j, False).wait_recv()

        @pl.when(s < places - 1)
        def _():
            halo(f, j, True).wait_recv()

    def finish_halo(f, j):
        @pl.when(s > 0)
        def _():
            halo(f, j, True).wait_send()

        @pl.when(s < places - 1)
        def _():
            halo(f, j, False).wait_send()

    for f in range(frames):
        send_halo(f, 0)
    other_core = b + 1 - 2 * core
    cot_copy = remote(cot_in.at[:, pl.ds(pl.multiple_of((1 - core) * half, half), half)], cot.at[1],
                      s_cs.at[0], s_cr.at[0], "batch", other_core)
    cot_copy.start()

    @pl.when(s == 0)
    def _():
        xx[:, 0] = jnp.zeros((frames, ranks, blk, depth), BF)

    @pl.when(s == places - 1)
    def _():
        xx[:, chunks + 1] = jnp.zeros((frames, ranks, blk, depth), BF)

    lane = lax.broadcasted_iota(jnp.int32, (1, LANES), 1)
    first_head = (lane < HEAD_DIM).astype(F32)
    masks = (first_head.astype(BF), (1.0 - first_head).astype(BF))
    head = lax.broadcasted_iota(jnp.int32, (depth, LANES), 0) // HEAD_DIM
    gather[...] = (head == lax.broadcasted_iota(jnp.int32, (depth, LANES), 1)).astype(F32).astype(BF)
    head = lax.broadcasted_iota(jnp.int32, (LANES, depth), 1) // HEAD_DIM
    spread[...] = (head == lax.broadcasted_iota(jnp.int32, (LANES, depth), 0)).astype(F32).astype(BF)
    for f in range(frames):
        for chunk in range(chunks):
            shape = (span, 3 * span)
            q_row = chunk * HALO + lax.broadcasted_iota(jnp.int32, shape, 0) % blk // pc
            k_at = lax.broadcasted_iota(jnp.int32, shape, 1)
            k_row = (chunk - 1 + k_at // span) * HALO + k_at % blk // pc
            place = s * rows + k_row
            kept = (jnp.abs(k_row - q_row) <= reach_ref[f]) & (place >= 0) & (place < rows * places)
            bias[f, chunk] = jnp.where(kept, 0.0, -1e30)

    def normalize(values, gain):
        widened = values.astype(F32)
        scaled = widened * lax.rsqrt(jnp.mean(widened * widened, axis=-1, keepdims=True) + FLOOR)
        return (scaled * gain[...]).astype(BF)

    def project_spatial(blocks, first):
        for i, (f, slot, source) in enumerate(blocks):
            nb[i * blk:(i + 1) * blk] = normalize(xx[f, slot, source], gain_one)
        count = len(blocks) * blk
        per = depth // TILE

        def step(i, carry):
            at = pl.ds(pl.multiple_of(i * TILE, TILE), TILE)
            lanes = pl.ds(pl.multiple_of(i % per * TILE, TILE), TILE)
            got = jnp.dot(nb[:count], w1[:, at], preferred_element_type=F32).astype(BF)
            for k, (f, slot, source) in enumerate(blocks):
                pr[i // per, f, slot, source, :, lanes] = got[k * blk:(k + 1) * blk]
            return carry

        lax.fori_loop(first * per, 3 * per, step, 0)

    own = range(1, chunks + 1)
    ends = (0, chunks + 1)
    ready(*[f"x{f}" for f in range(frames)], "w10", "w11", "w12")
    project_spatial([(f, slot, t) for f in range(frames) for slot in own], 0)
    for f in range(frames):
        wait_halo(f, 0)
    project_spatial([(f, slot, t) for f in range(frames) for slot in ends], 1)
    for f in range(frames):
        for j in range(1, ranks):
            x_copies[f, j].wait_recv()
            send_halo(f, j)
        project_spatial([(f, slot, (t - j) % ranks) for j in range(1, ranks) for slot in own], 0)

    def attend_spatial(f):
        ones = jnp.ones((3 * span, LANES), BF)

        def pair_step(pair, carry):
            at = pl.ds(pl.multiple_of(pair * LANES, LANES), LANES)
            for chunk in range(chunks):
                q = pr[0, f, 1 + chunk, :, :, at].reshape(span, LANES) * BF(SCALE)
                both = jnp.concatenate([q * masks[0], q * masks[1]], axis=0)
                k = pr[1, f, chunk:chunk + 3, :, :, at].reshape(3 * span, LANES)
                v = pr[2, f, chunk:chunk + 3, :, :, at].reshape(3 * span, LANES)
                sc = lax.dot_general(both, k, (((1,), (1,)), ((), ())), preferred_element_type=F32)
                sc = sc + jnp.concatenate([bias[f, chunk], bias[f, chunk]], axis=0)
                p = jnp.exp(sc - jnp.max(sc, axis=-1, keepdims=True)).astype(BF)
                o = jnp.dot(p, jnp.concatenate([v, ones], axis=1), preferred_element_type=F32)
                o = o[:, :LANES] / o[:, LANES:]
                ctx1[chunk * span:(chunk + 1) * span, at] = jnp.where(lane < HEAD_DIM, o[:span], o[span:]).astype(BF)
            return carry

        lax.fori_loop(0, depth // LANES, pair_step, 0)

    def merge_spatial(f):
        def step(i, carry):
            at = pl.ds(pl.multiple_of(i * TILE, TILE), TILE)
            got = jnp.dot(ctx1[...], o1[:, at], preferred_element_type=F32)
            for chunk in range(chunks):
                for source in range(ranks):
                    base = chunk * span + source * blk
                    total = (got[base:base + blk] + xx[f, 1 + chunk, source, :, at].astype(F32)).astype(BF)
                    for r in range(HALO):
                        row = (chunk * HALO + r) * cols + source * pc
                        mid[f, row:row + pc, at] = total[r * pc:(r + 1) * pc]
            return carry

        lax.fori_loop(0, depth // TILE, step, 0)

    ready("o1")
    m_copies = {}
    for f in range(frames):
        for j in range(1, ranks):
            wait_halo(f, j)
        project_spatial([(f, slot, (t - j) % ranks) for j in range(1, ranks) for slot in ends], 1)
        attend_spatial(f)
        merge_spatial(f)
        for j in range(1, ranks):
            copy = remote(mid.at[f], mids.at[j - 1, f], s_ms.at[f, j - 1], s_mr.at[f, j - 1], "tm", (t + j) % ranks)
            copy.start()
            m_copies[f, j] = copy

    def project_temporal(read, key, query):
        for i in range(0, tokens, 64):
            nb[i:i + 64] = normalize(read(i, 64), gain_two)
        per = depth // TILE

        def make(dst, part):
            def step(i, carry):
                at = pl.ds(pl.multiple_of(part * depth + i * TILE, TILE), TILE)
                lanes = pl.ds(pl.multiple_of(i * TILE, TILE), TILE)
                dst[:, lanes] = jnp.dot(nb[:tokens], w2[:, at], preferred_element_type=F32).astype(BF)
                return carry
            return step

        if query is not None:
            lax.fori_loop(0, per, make(qs.at[query], 0), 0)
        lax.fori_loop(0, per, make(ks.at[key], 1), 0)
        lax.fori_loop(0, per, make(vs.at[key], 2), 0)

    ready("w2")
    for f in range(frames):
        project_temporal(lambda i, n, f=f: mid[f, i:i + n], f, f)
    for f in range(frames):
        for j in range(1, ranks):
            m_copies[f, j].wait_recv()
            project_temporal(lambda i, n, f=f, j=j: mids[j - 1, f, i:i + n], j * frames + f, None)

    k_order = [order_ref[(t - j) % ranks * frames + g] for j in range(ranks) for g in range(frames)]
    size = 32

    def attend_temporal(f):
        def step(i, carry):
            at = pl.ds(pl.multiple_of(i * size, size), size)
            q = qs[f, at] * BF(SCALE)
            scores = []
            for g in range(keys):
                sc = jnp.dot(q * ks[g, at], gather[...], preferred_element_type=F32)
                scores.append(sc + jnp.where(k_order[g] <= k_order[f], 0.0, -1e30))
            top_score = functools.reduce(jnp.maximum, scores)
            exps = [jnp.exp(sc - top_score) for sc in scores]
            scale = 1.0 / functools.reduce(jnp.add, exps)
            total = None
            for g in range(keys):
                w = jnp.dot((exps[g] * scale).astype(BF), spread[...], preferred_element_type=F32)
                term = w * vs[g, at].astype(F32)
                total = term if total is None else total + term
            ctx2[0, pl.ds(pl.multiple_of(f * tokens + i * size, size), size)] = total.astype(BF)
            return carry

        lax.fori_loop(0, tokens // size, step, 0)

    c_copies = []
    for f in range(frames):
        attend_temporal(f)
        at = slice(f * tokens, (f + 1) * tokens)
        copy = remote(ctx2.at[0, at], ctx2.at[1, at], s_cs.at[1 + f], s_cr.at[1 + f], "batch", other_core)
        copy.start()
        c_copies.append(copy)

    ready("cot", "o2")
    cot_copy.wait()
    for copy in c_copies:
        copy.wait()
    row_tile = 256

    def grad_step(i, carry):
        at = pl.ds(pl.multiple_of(i * row_tile, row_tile), row_tile)
        total = None
        for which in range(2):
            got = lax.dot_general(ctx2[which, :, at], cot[which], (((0,), (0,)), ((), ())),
                                  preferred_element_type=F32)
            total = got if total is None else total + got
        acc[at] = total.astype(BF)
        return carry

    lax.fori_loop(0, depth // row_tile, grad_step, 0)

    sems = iter(range(s_gs.shape[0]))

    def exchange(axis, me, count, pieces, dests, slots=None):
        copies = []
        for k in range(1, count):
            to = (me + k) % count
            n = next(sems)
            copy = remote(pieces(to), dests.at[k - 1], s_gs.at[n], s_gr.at[n], axis, to)
            copy.start()
            copies.append(copy)
        return copies

    def over_y(pieces, dests):
        copies = []
        for k in range(1, ny):
            to = (y + k) % ny
            n = next(sems)
            copy = remote(pieces(to), dests.at[k - 1], s_gs.at[n], s_gr.at[n], "batch", to * 2 + core)
            copy.start()
            copies.append(copy)
        return copies

    def wait(copies):
        for copy in copies:
            copy.wait()

    def rows_of(to):
        return pl.ds(pl.multiple_of(to * own_rows, own_rows), own_rows)

    def lanes_of(base, to):
        return pl.ds(pl.multiple_of(base + to * lane_part, lane_part), lane_part)

    one_x = exchange("tm", t, ranks, lambda to: acc.at[rows_of(to), 0:quarter], axr)
    two_y = over_y(lambda to: acc.at[:, lanes_of(quarter, to)], byr)

    for f in range(frames):
        def out_step(i, carry, f=f):
            at = pl.ds(pl.multiple_of(i * TILE, TILE), TILE)
            got = jnp.dot(ctx2[0, f * tokens:(f + 1) * tokens], o2[:, at], preferred_element_type=F32)
            outv[f, :, at] = (mid[f, :, at].astype(F32) + got).astype(BF)
            return carry

        lax.fori_loop(0, depth // TILE, out_step, 0)
    out_copy = pltpu.make_async_copy(outv, out, s_out)
    out_copy.start()

    def total_of(first, received, count):
        total = first.astype(F32)
        for k in range(count - 1):
            total = total + received[k].astype(F32)
        return total

    wait(one_x)
    a1[...] = total_of(acc[rows_of(t), 0:quarter], axr, ranks).astype(BF)
    one_y = over_y(lambda to: a1.at[:, lanes_of(0, to)], ayr)
    wait(two_y)
    b1[...] = total_of(acc[:, lanes_of(quarter, y)], byr, ny).astype(BF)
    two_x = exchange("tm", t, ranks, lambda to: b1.at[rows_of(to)], bxr)
    wait(one_y)
    zb[:, :lane_part] = total_of(a1[:, lanes_of(0, y)], ayr, ny).astype(BF)
    wait(two_x)
    zb[:, lane_part:] = total_of(b1[rows_of(t)], bxr, ranks).astype(BF)

    def block_of(to):
        return pl.ds(pl.multiple_of(to * piece_rows, piece_rows), piece_rows)

    wait(exchange("space", s, places, lambda to: zb.at[block_of(to)], zr))
    gp[...] = total_of(zb[block_of(s)], zr, places).astype(BF)
    last = exchange("batch", b, parts, lambda to: gp, gr)

    def place_piece(owner, value):
        base = owner % 2 * half + owner // 2 * lane_part
        grad[:, pl.ds(pl.multiple_of(base, lane_part), lane_part)] = value[:, :lane_part].astype(F32)
        grad[:, pl.ds(pl.multiple_of(base + quarter, lane_part), lane_part)] = value[:, lane_part:].astype(F32)

    place_piece(b, gp[...])
    for k, copy in enumerate(last):
        copy.wait()
        place_piece((b - 1 - k) % parts, gr[k])

    for copy in x_copies.values():
        copy.wait_send()
    for copy in m_copies.values():
        copy.wait_send()
    for f in range(frames):
        for j in range(ranks):
            finish_halo(f, j)
    out_copy.wait()


def per_device(clip_tokens, frame_order, row_reach, spatial_gain, spatial_heads, spatial_merge,
               temporal_gain, temporal_heads, temporal_merge, cotangent):
    ranks, places, parts = lax.axis_size("tm"), lax.axis_size("space"), lax.axis_size("batch")
    _, all_frames, rows, pc, depth = clip_tokens.shape
    frames, cols = all_frames // ranks, pc * ranks
    chunks, blk, tokens = rows // HALO, HALO * pc, rows * cols
    span = blk * ranks
    keys = ranks * frames
    ny = parts // 2
    half, quarter = depth // 2, depth // 4
    lane_part, own_rows = quarter // ny, depth // ranks
    piece_rows = own_rows // places
    dims = (ranks, places, parts, frames, chunks, pc, depth)
    anywhere = pl.BlockSpec(memory_space=pl.ANY)
    smem = pl.BlockSpec(memory_space=pltpu.SMEM)
    vmem = pl.BlockSpec(memory_space=pltpu.VMEM)
    dma = pltpu.SemaphoreType.DMA
    others = max(ranks - 1, 1)
    most = max(2 * frames * chunks, 2 * frames * 2, (ranks - 1) * max(chunks, 2)) * blk
    steps = 2 * (ranks - 1) + 2 * (ny - 1) + (places - 1) + (parts - 1)
    scratch = [
        pltpu.VMEM((frames, chunks + 2, ranks, blk, depth), BF),
        pltpu.VMEM((3, frames, chunks + 2, ranks, blk, depth), BF),
        pltpu.VMEM((max(most, tokens), depth), BF),
        pltpu.VMEM((depth, 3 * depth), BF),
        pltpu.VMEM((depth, depth), BF),
        pltpu.VMEM((depth, 3 * depth), BF),
        pltpu.VMEM((depth, depth), BF),
        pltpu.VMEM((tokens, depth), BF),
        pltpu.VMEM((frames, tokens, depth), BF),
        pltpu.VMEM((others, frames, tokens, depth), BF),
        pltpu.VMEM((frames, tokens, depth), BF),
        pltpu.VMEM((keys, tokens, depth), BF),
        pltpu.VMEM((keys, tokens, depth), BF),
        pltpu.VMEM((2, frames * tokens, depth), BF),
        pltpu.VMEM((2, frames * tokens, half), BF),
        pltpu.VMEM((depth, LANES), BF),
        pltpu.VMEM((LANES, depth), BF),
        pltpu.VMEM((frames, chunks, span, 3 * span), F32),
        pltpu.VMEM((depth, half), BF),
        pltpu.VMEM((others, own_rows, quarter), BF),
        pltpu.VMEM((own_rows, quarter), BF),
        pltpu.VMEM((max(ny - 1, 1), own_rows, lane_part), BF),
        pltpu.VMEM((max(ny - 1, 1), depth, lane_part), BF),
        pltpu.VMEM((depth, lane_part), BF),
        pltpu.VMEM((others, own_rows, lane_part), BF),
        pltpu.VMEM((own_rows, 2 * lane_part), BF),
        pltpu.VMEM((max(places - 1, 1), piece_rows, 2 * lane_part), BF),
        pltpu.VMEM((piece_rows, 2 * lane_part), BF),
        pltpu.VMEM((parts - 1, piece_rows, 2 * lane_part), BF),
        pltpu.VMEM((frames, tokens, depth), BF),
        dma((frames + 7,)),
        dma((frames, others)), dma((frames, others)),
        dma((2, frames, ranks)), dma((2, frames, ranks)),
        dma((frames, others)), dma((frames, others)),
        dma((1 + frames,)), dma((1 + frames,)),
        dma((steps,)), dma((steps,)),
        dma,
    ]
    out, grad = pl.pallas_call(
        functools.partial(block_kernel, dims),
        out_shape=(jax.ShapeDtypeStruct((frames, tokens, depth), BF),
                   jax.ShapeDtypeStruct((piece_rows, depth), F32)),
        in_specs=[anywhere, smem, smem, vmem, vmem] + [anywhere] * 5,
        out_specs=(anywhere, vmem),
        scratch_shapes=scratch,
        compiler_params=pltpu.CompilerParams(collective_id=0, has_side_effects=True,
                                             vmem_limit_bytes=67043328),
        name="block",
    )(clip_tokens.reshape(all_frames, chunks, blk, depth), frame_order.reshape(-1), row_reach.reshape(-1),
      spatial_gain.reshape(1, depth), temporal_gain.reshape(1, depth),
      spatial_heads, spatial_merge, temporal_heads, temporal_merge, cotangent.reshape(-1, depth))
    return out.reshape(1, frames, rows, cols, depth), grad


def solution(mesh):
    in_specs = (
        P("batch", None, "space", "tm", None),
        P("batch", None),
        P("batch", "tm"),
        P(),
        P(),
        P(),
        P(),
        P(),
        P(),
        P("batch", "tm", "space", None, None),
    )
    out_specs = (P("batch", "tm", "space", None, None), P(("tm", "space"), None))
    return jax.shard_map(per_device, mesh=mesh, in_specs=in_specs, out_specs=out_specs, check_vma=False)
```

```python
import functools

import jax
import jax.numpy as jnp
from jax import lax
from jax.experimental import pallas as pl
from jax.experimental.pallas import tpu as pltpu
from jax.sharding import PartitionSpec as P

HALO = 4
HEADS = 16
HEAD_DIM = 64
LANES = 128
TILE = 1024
PIECE = 64
UNROLL = 8
SCALE = HEAD_DIM ** (-0.5)
FLOOR = 0.5
BF = jnp.bfloat16
F32 = jnp.float32
MESH = pl.DeviceIdType.MESH


def block_kernel(dims, *refs):
    ranks, places, parts, frames, chunks, pc, depth = dims
    (clip, order_ref, reach_ref, gain_one, gain_two, w_one, m_one, w_two, m_two, cot_in,
     out, grad,
     xx, away_x, pr, nb, w1, o1, w2, o2, ctx1, mid, mids, qs, ks, vs, ctx2, cot, gather, spread, bias, accf, acc,
     xr_one, yr_one, one_x, one_y, xr_two, yr_two, two, zr, gp, gr,
     s_load, s_xs, s_xr, s_zs, s_zr, s_ms, s_mr, s_cs, s_cr, s_gs, s_gr, s_out) = refs
    blk = HALO * pc
    span = blk * ranks
    cols = pc * ranks
    tokens = chunks * span
    rows = chunks * HALO
    keys = ranks * frames
    half = depth // 2
    t, s, b = lax.axis_index("tm"), lax.axis_index("space"), lax.axis_index("batch")
    core, y = b % 2, b // 2
    ny = parts // 2

    loads = {}

    def load(name, src, dst):
        copy = pltpu.make_async_copy(src, dst, s_load.at[len(loads)])
        copy.start()
        loads[name] = copy

    def ready(*names):
        for name in names:
            loads[name].wait()

    def half_of(which):
        return pl.ds(pl.multiple_of(which * half, half), half)

    for f in range(frames):
        load(f"x{f}", clip.at[t * frames + f], xx.at[f, 1:chunks + 1, t])
        for j in range(1, ranks):
            load(f"y{f}{j}", clip.at[(t + j) % ranks * frames + f], away_x.at[j - 1, f])
    for part in range(3):
        load(f"w1{part}", w_one.at[:, part * depth:(part + 1) * depth], w1.at[:, part * depth:(part + 1) * depth])
    load("o1", m_one, o1)
    load("w2", w_two, w2)
    load("o2", m_two, o2)
    for f in range(frames):
        load(f"cot{f}", cot_in.at[f, :, :, half_of(core)], cot.at[0, :, f])

    barrier = pltpu.get_barrier_semaphore()
    for axis, me, count in (("tm", t, ranks), ("space", s, places), ("batch", b, parts)):
        for shift in range(1, count):
            pl.semaphore_signal(barrier, inc=1, device_id={axis: (me + shift) % count}, device_id_type=MESH)
    pl.semaphore_wait(barrier, ranks + places + parts - 3)

    ready(*[f"x{f}" for f in range(frames)], *[f"y{f}{j}" for f in range(frames) for j in range(1, ranks)])
    def remote(src, dst, send, recv, axis, to):
        return pltpu.make_async_remote_copy(src, dst, send, recv, device_id={axis: to}, device_id_type=MESH)

    x_copies = {}
    for f in range(frames):
        for chunk in range(chunks):
            for j in range(1, ranks):
                to = (t + j) % ranks
                copy = remote(away_x.at[j - 1, f, chunk], xx.at[f, 1 + chunk, t],
                              s_xs.at[f, chunk, j - 1], s_xr.at[f, chunk, j - 1], "tm", to)
                copy.start()
                x_copies[f, chunk, j] = copy

    def halo(f, j, up):
        source = (t - j) % ranks
        slot, dest = (1, chunks + 1) if up else (chunks, 0)
        return remote(xx.at[f, slot, source], xx.at[f, dest, source], s_zs.at[int(up), f, j], s_zr.at[int(up), f, j],
                      "space", (s - 1) if up else (s + 1))

    def send_halo(f, j, up):
        @pl.when((s > 0) if up else (s < places - 1))
        def _():
            halo(f, j, up).start()

    def wait_halo(f, j, sides=(False, True)):
        for up in sides:
            @pl.when((s < places - 1) if up else (s > 0))
            def _():
                halo(f, j, up).wait_recv()

    def finish_halo(f, j):
        @pl.when(s > 0)
        def _():
            halo(f, j, True).wait_send()

        @pl.when(s < places - 1)
        def _():
            halo(f, j, False).wait_send()

    def forward(f, chunk):
        for j in range(1, ranks):
            x_copies[f, chunk, j].wait_recv()
            if chunk == 0:
                send_halo(f, j, True)
            if chunk == chunks - 1:
                send_halo(f, j, False)
        if f + 1 < frames and chunk == 0:
            send_halo(f + 1, 0, True)
        if f + 1 < frames and chunk == chunks - 1:
            send_halo(f + 1, 0, False)

    send_halo(0, 0, True)
    send_halo(0, 0, False)
    other_core = b + 1 - 2 * core
    cot_copies = []
    for f in range(frames):
        copy = remote(cot_in.at[f, :, :, half_of(1 - core)], cot.at[1, :, f], s_cs.at[f], s_cr.at[f],
                      "batch", other_core)
        copy.start()
        cot_copies.append(copy)

    @pl.when(s == 0)
    def _():
        xx[:, 0] = jnp.zeros((frames, ranks, blk, depth), BF)

    @pl.when(s == places - 1)
    def _():
        xx[:, chunks + 1] = jnp.zeros((frames, ranks, blk, depth), BF)

    lane = lax.broadcasted_iota(jnp.int32, (1, LANES), 1)
    first_head = (lane < HEAD_DIM).astype(F32)
    masks = (first_head.astype(BF), (1.0 - first_head).astype(BF))
    for f in range(frames):
        for chunk in range(chunks):
            shape = (span, 3 * span)
            q_row = chunk * HALO + lax.broadcasted_iota(jnp.int32, shape, 0) % blk // pc
            k_at = lax.broadcasted_iota(jnp.int32, shape, 1)
            k_row = (chunk - 1 + k_at // span) * HALO + k_at % blk // pc
            place = s * rows + k_row
            kept = (jnp.abs(k_row - q_row) <= reach_ref[f]) & (place >= 0) & (place < rows * places)
            bias[f, chunk] = jnp.where(kept, 0.0, -1e30)

    def normalize(values, gain):
        widened = values.astype(F32)
        scaled = widened * lax.rsqrt(jnp.mean(widened * widened, axis=-1, keepdims=True) + FLOOR)
        return (scaled * gain[...]).astype(BF)

    def project_spatial(blocks, first):
        for i, (f, slot, source) in enumerate(blocks):
            nb[i * blk:(i + 1) * blk] = normalize(xx[f, slot, source], gain_one)
        count = len(blocks) * blk
        per = depth // TILE

        def step(i, carry):
            at = pl.ds(pl.multiple_of(i * TILE, TILE), TILE)
            lanes = pl.ds(pl.multiple_of(i % per * TILE, TILE), TILE)
            got = jnp.dot(nb[:count], w1[:, at], preferred_element_type=F32).astype(BF)
            for k, (f, slot, source) in enumerate(blocks):
                pr[i // per, f, slot, source, :, lanes] = got[k * blk:(k + 1) * blk]
            return carry

        lax.fori_loop(first * per, 3 * per, step, 0)

    own = range(1, chunks + 1)
    ends = (0, chunks + 1)
    away = range(1, ranks)

    def attend_spatial(f, chunk):
        ones = jnp.ones((3 * span, LANES), BF)

        def pair_step(i, carry):
            for u in range(UNROLL):
                at = pl.ds(pl.multiple_of((UNROLL * i + u) * LANES, LANES), LANES)
                q = pr[0, f, 1 + chunk, :, :, at].reshape(span, LANES) * BF(SCALE)
                both = jnp.concatenate([q * masks[0], q * masks[1]], axis=0)
                k = pr[1, f, chunk:chunk + 3, :, :, at].reshape(3 * span, LANES)
                v = pr[2, f, chunk:chunk + 3, :, :, at].reshape(3 * span, LANES)
                sc = lax.dot_general(both, k, (((1,), (1,)), ((), ())), preferred_element_type=F32)
                sc = sc + jnp.concatenate([bias[f, chunk], bias[f, chunk]], axis=0)
                p = jnp.exp(sc - jnp.max(sc, axis=-1, keepdims=True)).astype(BF)
                o = jnp.dot(p, jnp.concatenate([v, ones], axis=1), preferred_element_type=F32)
                o = jnp.where(jnp.concatenate([lane, lane], axis=1) % LANES < HEAD_DIM, o[:span], o[span:])
                ctx1[:, at] = (o[:, :LANES] / o[:, LANES:]).astype(BF)
            return carry

        lax.fori_loop(0, depth // LANES // UNROLL, pair_step, 0)

    m_copies = {}

    def merge_spatial(f, chunk):
        def step(i, carry):
            at = pl.ds(pl.multiple_of(i * TILE, TILE), TILE)
            got = jnp.dot(ctx1[...], o1[:, at], preferred_element_type=F32)
            for source in range(ranks):
                base = source * blk
                total = (got[base:base + blk] + xx[f, 1 + chunk, source, :, at].astype(F32)).astype(BF)
                for r in range(HALO):
                    row = (chunk * HALO + r) * cols + source * pc
                    mid[f, row:row + pc, at] = total[r * pc:(r + 1) * pc]
            return carry

        lax.fori_loop(0, depth // TILE, step, 0)
        for piece in range(chunk * span // PIECE, (chunk + 1) * span // PIECE):
            at = slice(piece * PIECE, (piece + 1) * PIECE)
            for j in away:
                copy = remote(mid.at[f, at], mids.at[j - 1, f, at], s_ms.at[f, piece, j - 1],
                              s_mr.at[f, piece, j - 1], "tm", (t + j) % ranks)
                copy.start()
                m_copies[f, piece, j] = copy

    ready("w10", "w11", "w12")
    project_spatial([(f, slot, t) for f in range(frames) for slot in own], 0)
    for chunk in range(chunks - 1):
        forward(0, chunk)
    wait_halo(0, 0)
    project_spatial([(0, slot, t) for slot in ends], 1)
    forward(0, chunks - 1)
    project_spatial([(0, slot, (t - j) % ranks) for j in away for slot in own], 0)
    ready("o1")
    for f in range(frames):
        if f == 0:
            for j in away:
                wait_halo(f, j, (True,))
            project_spatial([(f, chunks + 1, (t - j) % ranks) for j in away], 1)
        else:
            for j in range(ranks):
                wait_halo(f, j)
            project_spatial([(f, slot, (t - j) % ranks) for j in range(ranks) for slot in ends], 1)
        if f + 1 < frames:
            for chunk in range(chunks - 1):
                forward(f + 1, chunk)
        for chunk in reversed(range(chunks)):
            if f == 0 and chunk == 0:
                for j in away:
                    wait_halo(f, j, (False,))
                project_spatial([(f, 0, (t - j) % ranks) for j in away], 1)
            attend_spatial(f, chunk)
            merge_spatial(f, chunk)
            if f + 1 < frames and chunk == chunks - 1:
                forward(f + 1, chunks - 1)
        if f + 1 < frames:
            project_spatial([(f + 1, slot, (t - j) % ranks) for j in away for slot in own], 0)

    head = lax.broadcasted_iota(jnp.int32, (depth, LANES), 0) // HEAD_DIM
    gather[...] = (head == lax.broadcasted_iota(jnp.int32, (depth, LANES), 1)).astype(F32).astype(BF)
    head = lax.broadcasted_iota(jnp.int32, (LANES, depth), 1) // HEAD_DIM
    spread[...] = (head == lax.broadcasted_iota(jnp.int32, (LANES, depth), 0)).astype(F32).astype(BF)

    def project_temporal(sources, parts_of, count):
        for i, read in enumerate(sources):
            nb[i * PIECE:(i + 1) * PIECE] = normalize(read(), gain_two)
        per = depth // TILE

        def make(dst, part):
            def step(i, carry):
                at = pl.ds(pl.multiple_of(part * depth + i * TILE, TILE), TILE)
                lanes = pl.ds(pl.multiple_of(i * TILE, TILE), TILE)
                got = jnp.dot(nb[:len(sources) * PIECE], w2[:, at], preferred_element_type=F32).astype(BF)
                for k, ref in enumerate(dst):
                    ref[:, lanes] = got[k * count:(k + 1) * count]
                return carry
            return step

        for part, dst in parts_of:
            lax.fori_loop(0, per, make(dst, part), 0)

    pieces = tokens // PIECE
    spot = lambda piece: slice(piece * PIECE, (piece + 1) * PIECE)
    ready("w2")
    for f in range(frames):
        project_temporal([lambda f=f, p=p: mid[f, spot(p)] for p in range(pieces)],
                         [(0, [qs.at[f]]), (1, [ks.at[f]]), (2, [vs.at[f]])], tokens)
    for f in range(frames - 1):
        for j in away:
            for p in range(pieces):
                m_copies[f, p, j].wait_recv()
            project_temporal([lambda f=f, j=j, p=p: mids[j - 1, f, spot(p)] for p in range(pieces)],
                             [(1, [ks.at[j * frames + f]]), (2, [vs.at[j * frames + f]])], tokens)

    k_order = [order_ref[(t - j) % ranks * frames + g] for j in range(ranks) for g in range(frames)]
    size = max(16, min(PIECE, 256 // (frames * keys)))
    pairs = [(f, g) for f in range(frames) for g in range(keys)]

    def attend_temporal(first, count):
        per = PIECE // size

        def step(i, carry):
            at = pl.ds(pl.multiple_of(first * PIECE + i * size, size), size)
            piece, within = first + i // per, i % per
            q = [qs[f, at] * BF(SCALE) for f in range(frames)]
            products = jnp.concatenate([q[f] * ks[g, at] for f, g in pairs], axis=0)
            scores = jnp.dot(products, gather[...], preferred_element_type=F32)
            scores = {pair: scores[n * size:(n + 1) * size] for n, pair in enumerate(pairs)}
            weights = []
            for f in range(frames):
                kept = [scores[f, g] + jnp.where(k_order[g] <= k_order[f], 0.0, -1e30) for g in range(keys)]
                top_score = functools.reduce(jnp.maximum, kept)
                exps = [jnp.exp(sc - top_score) for sc in kept]
                scale = 1.0 / functools.reduce(jnp.add, exps)
                weights += [(e * scale).astype(BF) for e in exps]
            spreads = jnp.dot(jnp.concatenate(weights, axis=0), spread[...], preferred_element_type=F32)
            for f in range(frames):
                total = None
                for g in range(keys):
                    n = f * keys + g
                    term = spreads[n * size:(n + 1) * size] * vs[g, at].astype(F32)
                    total = term if total is None else total + term
                ctx2[0, piece, f, pl.ds(pl.multiple_of(within * size, size), size)] = total.astype(BF)
            return carry

        lax.fori_loop(0, count * per, step, 0)

    row_tile = 1024
    sub = depth // (ranks * places * ny)
    stacked = frames * PIECE

    def add_gradient(terms, first, final):
        def step(i, carry):
            at = pl.ds(pl.multiple_of(i * row_tile, row_tile), row_tile)
            left = jnp.concatenate([ctx2[w, p, :, :, at].reshape(stacked, row_tile) for w, p in terms], axis=0)
            right = jnp.concatenate([cot[w, p].reshape(stacked, half) for w, p in terms], axis=0)
            got = lax.dot_general(left, right, (((0,), (0,)), ((), ())), preferred_element_type=F32)
            if not first:
                got = got + accf[at]
            if final:
                acc[at] = got.astype(BF)
            else:
                accf[at] = got
            return carry

        lax.fori_loop(0, depth // row_tile, step, 0)

    c_copies = []
    final = frames - 1
    ready(*[f"cot{f}" for f in range(frames)])
    for copy in cot_copies:
        copy.wait()
    per_chunk = span // PIECE
    arrival = [c * per_chunk + i for c in reversed(range(chunks)) for i in range(per_chunk)]
    groups = [arrival[n:n + per_chunk] for n in range(0, pieces - per_chunk, per_chunk)]
    groups += [[p] for p in arrival[-per_chunk:]]
    ahead = []
    for number, group in enumerate(groups):
        for p in group:
            for j in away:
                m_copies[final, p, j].wait_recv()
        lo, n = group[0], len(group)
        whole = slice(lo * PIECE, (lo + n) * PIECE)
        for j in away:
            project_temporal([lambda j=j, p=p: mids[j - 1, final, spot(p)] for p in group],
                             [(1, [ks.at[j * frames + final, whole]]), (2, [vs.at[j * frames + final, whole]])],
                             n * PIECE)
        attend_temporal(lo, n)
        copy = remote(ctx2.at[0, lo:lo + n], ctx2.at[1, lo:lo + n], s_cs.at[frames + number],
                      s_cr.at[frames + number], "batch", other_core)
        copy.start()
        c_copies.append(copy)
        if number:
            c_copies[number - 1].wait_recv()
        add_gradient([(0, p) for p in group] + [(1, p) for p in ahead], number == 0, False)
        ahead = group
    c_copies[-1].wait_recv()
    add_gradient([(1, p) for p in ahead], False, True)

    sems = iter(range(s_gs.shape[0]))

    def exchange(axis, me, count, to_device, source, dests):
        copies = []
        for k in range(1, count):
            to = (me + k) % count
            n = next(sems)
            copy = remote(source(to), dests.at[k - 1], s_gs.at[n], s_gr.at[n], axis, to_device(to))
            copy.start()
            copies.append(copy)
        return copies

    def over_x(source, dests):
        return exchange("tm", t, ranks, lambda to: to, source, dests)

    def over_y(source, dests):
        return exchange("batch", y, ny, lambda to: to * 2 + core, source, dests)

    def over_z(source, dests):
        return exchange("space", s, places, lambda to: to, source, dests)

    def wait(copies):
        for copy in copies:
            copy.wait()

    def total_of(first, received, count):
        total = first.astype(F32)
        for k in range(count - 1):
            total = total + received[k].astype(F32)
        return total

    stage_one = []
    grid = acc.reshape(ranks, places, ny, sub, half)
    column = lambda n: slice(n * LANES, (n + 1) * LANES)
    count = half // LANES
    for n in range(count):
        if n % 2 == 0:
            stage_one.append(over_x(lambda to, n=n: grid.at[to, :, :, :, column(n)], xr_one.at[n // 2]))
        else:
            stage_one.append(over_y(lambda to, n=n: grid.at[:, :, to, :, column(n)], yr_one.at[n // 2]))

    ready("o2")

    def out_step(i, carry):
        at = pl.ds(pl.multiple_of(i * TILE, TILE), TILE)
        got = jnp.dot(ctx2[0].reshape(frames * tokens, depth), o2[:, at], preferred_element_type=F32)
        for p in range(pieces):
            for f in range(frames):
                base = (p * frames + f) * PIECE
                qs[f, spot(p), at] = (mid[f, spot(p), at].astype(F32) + got[base:base + PIECE]).astype(BF)
        return carry

    lax.fori_loop(0, depth // TILE, out_step, 0)
    out_copy = pltpu.make_async_copy(qs, out, s_out)
    out_copy.start()

    stage_two = []
    for n in range(count):
        wait(stage_one[n])
        k = n // 2
        if n % 2 == 0:
            one_x[k] = total_of(grid[t, :, :, :, column(n)], xr_one.at[k], ranks).astype(BF)
            stage_two.append(over_y(lambda to, k=k: one_x.at[k, :, to], yr_two.at[k]))
        else:
            one_y[k] = total_of(grid[:, :, y, :, column(n)], yr_one.at[k], ny).astype(BF)
            stage_two.append(over_x(lambda to, k=k: one_y.at[k, to], xr_two.at[k]))
    stage_three = []
    for n in range(count):
        wait(stage_two[n])
        k = n // 2
        if n % 2 == 0:
            two[n] = total_of(one_x[k, :, y], yr_two.at[k], ny).astype(BF)
        else:
            two[n] = total_of(one_y[k, t], xr_two.at[k], ranks).astype(BF)
        stage_three.append(over_z(lambda to, n=n: two.at[n, to], zr.at[n]))
    for n in range(count):
        wait(stage_three[n])
        gp[:, column(n)] = total_of(two[n, s], zr.at[n], places).astype(BF)
    last = exchange("batch", b, parts, lambda to: to, lambda to: gp, gr)

    def place_piece(owner, value):
        grad[pl.ds(pl.multiple_of(owner // 2 * sub, sub), sub), half_of(owner % 2)] = value.astype(F32)

    place_piece(b, gp[...])
    for k, copy in enumerate(last):
        copy.wait()
        place_piece((b - 1 - k) % parts, gr[k])

    for copies in (x_copies, m_copies):
        for copy in copies.values():
            copy.wait_send()
    for copy in c_copies:
        copy.wait_send()
    for f in range(frames):
        for j in range(ranks):
            finish_halo(f, j)
    out_copy.wait()


def per_device(clip_tokens, frame_order, row_reach, spatial_gain, spatial_heads, spatial_merge,
               temporal_gain, temporal_heads, temporal_merge, cotangent):
    ranks, places, parts = lax.axis_size("tm"), lax.axis_size("space"), lax.axis_size("batch")
    _, all_frames, rows, pc, depth = clip_tokens.shape
    frames, cols = all_frames // ranks, pc * ranks
    chunks, blk, tokens = rows // HALO, HALO * pc, rows * cols
    span = blk * ranks
    keys = ranks * frames
    ny = parts // 2
    half = depth // 2
    sub = depth // (ranks * places * ny)
    pieces = tokens // PIECE
    chunks_of = half // LANES
    pairs = chunks_of // 2
    dims = (ranks, places, parts, frames, chunks, pc, depth)
    anywhere = pl.BlockSpec(memory_space=pl.ANY)
    smem = pl.BlockSpec(memory_space=pltpu.SMEM)
    vmem = pl.BlockSpec(memory_space=pltpu.VMEM)
    dma = pltpu.SemaphoreType.DMA
    others, ny_others = max(ranks - 1, 1), max(ny - 1, 1)
    most = max(frames * chunks * blk, 2 * ranks * blk, (ranks - 1) * max(chunks, 2) * blk,
               tokens)
    steps = pairs * 2 * (ranks - 1) + pairs * 2 * (ny - 1) + chunks_of * (places - 1) + (parts - 1)
    scratch = [
        pltpu.VMEM((frames, chunks + 2, ranks, blk, depth), BF),
        pltpu.VMEM((others, frames, chunks, blk, depth), BF),
        pltpu.VMEM((3, frames, chunks + 2, ranks, blk, depth), BF),
        pltpu.VMEM((most, depth), BF),
        pltpu.VMEM((depth, 3 * depth), BF),
        pltpu.VMEM((depth, depth), BF),
        pltpu.VMEM((depth, 3 * depth), BF),
        pltpu.VMEM((depth, depth), BF),
        pltpu.VMEM((span, depth), BF),
        pltpu.VMEM((frames, tokens, depth), BF),
        pltpu.VMEM((others, frames, tokens, depth), BF),
        pltpu.VMEM((frames, tokens, depth), BF),
        pltpu.VMEM((keys, tokens, depth), BF),
        pltpu.VMEM((keys, tokens, depth), BF),
        pltpu.VMEM((2, pieces, frames, PIECE, depth), BF),
        pltpu.VMEM((2, pieces, frames, PIECE, half), BF),
        pltpu.VMEM((depth, LANES), BF),
        pltpu.VMEM((LANES, depth), BF),
        pltpu.VMEM((frames, chunks, span, 3 * span), F32),
        pltpu.VMEM((depth, half), F32),
        pltpu.VMEM((depth, half), BF),
        pltpu.VMEM((pairs, others, places, ny, sub, LANES), BF),
        pltpu.VMEM((pairs, ny_others, ranks, places, sub, LANES), BF),
        pltpu.VMEM((pairs, places, ny, sub, LANES), BF),
        pltpu.VMEM((pairs, ranks, places, sub, LANES), BF),
        pltpu.VMEM((pairs, others, places, sub, LANES), BF),
        pltpu.VMEM((pairs, ny_others, places, sub, LANES), BF),
        pltpu.VMEM((chunks_of, places, sub, LANES), BF),
        pltpu.VMEM((chunks_of, max(places - 1, 1), sub, LANES), BF),
        pltpu.VMEM((sub, half), BF),
        pltpu.VMEM((parts - 1, sub, half), BF),
        dma((2 * frames + 6 + (ranks - 1) * frames,)),
        dma((frames, chunks, others)), dma((frames, chunks, others)),
        dma((2, frames, ranks)), dma((2, frames, ranks)),
        dma((frames, pieces, others)), dma((frames, pieces, others)),
        dma((frames + pieces,)), dma((frames + pieces,)),
        dma((steps,)), dma((steps,)),
        dma,
    ]
    out, grad = pl.pallas_call(
        functools.partial(block_kernel, dims),
        out_shape=(jax.ShapeDtypeStruct((frames, tokens, depth), BF),
                   jax.ShapeDtypeStruct((ny * sub, depth), F32)),
        in_specs=[anywhere, smem, smem, vmem, vmem] + [anywhere] * 5,
        out_specs=(anywhere, vmem),
        scratch_shapes=scratch,
        compiler_params=pltpu.CompilerParams(collective_id=0, has_side_effects=True,
                                             vmem_limit_bytes=67043328),
        name="block",
    )(clip_tokens.reshape(all_frames, chunks, blk, depth), frame_order.reshape(-1), row_reach.reshape(-1),
      spatial_gain.reshape(1, depth), temporal_gain.reshape(1, depth),
      spatial_heads, spatial_merge, temporal_heads, temporal_merge, cotangent.reshape(frames, pieces, PIECE, depth))
    return out.reshape(1, frames, rows, cols, depth), grad


def solution(mesh):
    in_specs = (
        P("batch", None, "space", "tm", None),
        P("batch", None),
        P("batch", "tm"),
        P(),
        P(),
        P(),
        P(),
        P(),
        P(),
        P("batch", "tm", "space", None, None),
    )
    out_specs = (P("batch", "tm", "space", None, None), P(("tm", "space"), None))
    return jax.shard_map(per_device, mesh=mesh, in_specs=in_specs, out_specs=out_specs, check_vma=False)
```

```python
import functools

import jax
import jax.numpy as jnp
from jax import lax
from jax.experimental import pallas as pl
from jax.experimental.pallas import tpu as pltpu
from jax.sharding import PartitionSpec as P

HALO = 4
HEADS = 16
HEAD_DIM = 64
LANES = 128
TILE = 1024
UNROLL = 8
SCALE = HEAD_DIM ** (-0.5)
FLOOR = 0.5
BF = jnp.bfloat16
F32 = jnp.float32
MESH = pl.DeviceIdType.MESH


def block_kernel(dims, *refs):
    ranks, places, parts, frames, chunks, pc, depth, inner = dims
    every = (slice(None), slice(None))
    (clip, order_ref, reach_ref, gain_one, gain_two, w_one, m_one, w_two, m_two, cot_in,
     out, grad,
     xx, away_x, pr, nb, w1, o1, w2, o2, ctx1, mid, mids, qkv, ctx2, cot, gather, spread, bias, accf, acc,
     xr_one, yr_one, one_x, one_y, xr_two, yr_two, two, zr, gp, gr, sent,
     s_load, s_xs, s_xr, s_zs, s_zr, s_ms, s_mr, s_ts, s_tr, s_cs, s_cr, s_os, s_or, s_gs, s_gr) = refs
    blk = HALO * pc
    span = blk * ranks
    rows = chunks * HALO
    keys = ranks * frames
    half = depth // 2
    t, s, b = lax.axis_index("tm"), lax.axis_index("space"), lax.axis_index("batch")
    core, y = b % 2, b // 2
    ny = parts // 2

    loads = {}

    def load(name, src, dst):
        copy = pltpu.make_async_copy(src, dst, s_load.at[len(loads)])
        copy.start()
        loads[name] = copy

    def ready(*names):
        for name in names:
            loads[name].wait()

    def half_of(which):
        return pl.ds(pl.multiple_of(which * half, half), half)

    for f in range(frames):
        load(f"x{f}", clip.at[t * frames + f], xx.at[f, 1:chunks + 1, t])
        for j in range(1, ranks):
            load(f"y{f}{j}", clip.at[(t + j) % ranks * frames + f], away_x.at[j - 1, f])
    for part in range(3):
        load(f"w1{part}", w_one.at[:, part * depth:(part + 1) * depth], w1.at[:, part * depth:(part + 1) * depth])
    load("o1", m_one, o1)
    load("w2", w_two, w2)
    load("o2", m_two, o2)
    for f in range(frames):
        load(f"cot{f}", cot_in.at[f, :, :, t, :, half_of(core)], cot.at[0, :, f])

    barrier = pltpu.get_barrier_semaphore()
    for axis, me, count in (("tm", t, ranks), ("space", s, places), ("batch", b, parts)):
        for shift in range(1, count):
            pl.semaphore_signal(barrier, inc=1, device_id={axis: (me + shift) % count}, device_id_type=MESH)
    other_core = b + 1 - 2 * core
    for j in range(1, ranks):
        pl.semaphore_signal(barrier, inc=1, device_id={"tm": (t + j) % ranks, "batch": other_core},
                            device_id_type=MESH)
    pl.semaphore_wait(barrier, 2 * ranks + places + parts - 4)

    ready(*[f"x{f}" for f in range(frames)], *[f"y{f}{j}" for f in range(frames) for j in range(1, ranks)])
    def remote(src, dst, send, recv, axis, to):
        return pltpu.make_async_remote_copy(src, dst, send, recv, device_id={axis: to}, device_id_type=MESH)

    x_copies = {}
    for f in range(frames):
        for chunk in range(chunks):
            for j in range(1, ranks):
                to = (t + j) % ranks
                copy = remote(away_x.at[j - 1, f, chunk], xx.at[f, 1 + chunk, t],
                              s_xs.at[f, chunk, j - 1], s_xr.at[f, chunk, j - 1], "tm", to)
                copy.start()
                x_copies[f, chunk, j] = copy

    def halo(f, j, up):
        source = (t - j) % ranks
        slot, dest = (1, chunks + 1) if up else (chunks, 0)
        return remote(xx.at[f, slot, source], xx.at[f, dest, source], s_zs.at[int(up), f, j], s_zr.at[int(up), f, j],
                      "space", (s - 1) if up else (s + 1))

    def send_halo(f, j, up):
        @pl.when((s > 0) if up else (s < places - 1))
        def _():
            halo(f, j, up).start()

    def wait_halo(f, j, sides=(False, True)):
        for up in sides:
            @pl.when((s < places - 1) if up else (s > 0))
            def _():
                halo(f, j, up).wait_recv()

    def finish_halo(f, j):
        @pl.when(s > 0)
        def _():
            halo(f, j, True).wait_send()

        @pl.when(s < places - 1)
        def _():
            halo(f, j, False).wait_send()

    def forward(f, chunk):
        for j in range(1, ranks):
            x_copies[f, chunk, j].wait_recv()
            if chunk == 0:
                send_halo(f, j, True)
            if chunk == chunks - 1:
                send_halo(f, j, False)
        if f + 1 < frames and chunk == 0:
            send_halo(f + 1, 0, True)
        if f + 1 < frames and chunk == chunks - 1:
            send_halo(f + 1, 0, False)

    send_halo(0, 0, True)
    send_halo(0, 0, False)
    cot_copies = []

    def send_cotangent(chunk, shifts):
        for j in shifts:
            to = (t + j) % ranks
            for which, core_to in ((0, core), (1, 1 - core)):
                if j == 0 and which == 0:
                    continue
                copy = pltpu.make_async_remote_copy(
                    cot_in.at[:, chunk, :, to, :, half_of(core_to)],
                    cot.at[which, chunk, j * frames:(j + 1) * frames],
                    s_ts.at[which, chunk, j], s_tr.at[which, chunk, j],
                    device_id={"tm": to, "batch": b - core + core_to}, device_id_type=MESH)
                copy.start()
                cot_copies.append((chunk, copy))

    order = list(reversed(range(chunks)))
    for chunk in order:
        send_cotangent(chunk, range(1))
    for chunk in order[:-1]:
        send_cotangent(chunk, range(1, ranks))

    @pl.when(s == 0)
    def _():
        xx[:, 0] = jnp.zeros((frames, ranks, blk, depth), BF)

    @pl.when(s == places - 1)
    def _():
        xx[:, chunks + 1] = jnp.zeros((frames, ranks, blk, depth), BF)

    lane = lax.broadcasted_iota(jnp.int32, (1, LANES), 1)
    first_head = (lane < HEAD_DIM).astype(F32)
    masks = (first_head.astype(BF), (1.0 - first_head).astype(BF))
    for f in range(frames):
        for chunk in range(chunks):
            shape = (span, 3 * span)
            q_row = chunk * HALO + lax.broadcasted_iota(jnp.int32, shape, 0) % blk // pc
            k_at = lax.broadcasted_iota(jnp.int32, shape, 1)
            k_row = (chunk - 1 + k_at // span) * HALO + k_at % blk // pc
            place = s * rows + k_row
            kept = (jnp.abs(k_row - q_row) <= reach_ref[f]) & (place >= 0) & (place < rows * places)
            bias[f, chunk] = jnp.where(kept, 0.0, -1e30)

    def normalize(values, gain):
        widened = values.astype(F32)
        scaled = widened * lax.rsqrt(jnp.mean(widened * widened, axis=-1, keepdims=True) + FLOOR)
        return (scaled * gain[...]).astype(BF)

    def project_spatial(blocks, first):
        for i, (f, slot, source) in enumerate(blocks):
            nb[i * blk:(i + 1) * blk] = normalize(xx[f, slot, source], gain_one)
        count = len(blocks) * blk
        per = depth // TILE

        def step(i, carry):
            at = pl.ds(pl.multiple_of(i * TILE, TILE), TILE)
            lanes = pl.ds(pl.multiple_of(i % per * TILE, TILE), TILE)
            got = jnp.dot(nb[:count], w1[:, at], preferred_element_type=F32).astype(BF)
            for k, (f, slot, source) in enumerate(blocks):
                pr[i // per, f, slot, source, :, lanes] = got[k * blk:(k + 1) * blk]
            return carry

        lax.fori_loop(first * per, 3 * per, step, 0, unroll=True)

    own = range(1, chunks + 1)
    ends = (0, chunks + 1)
    away = range(1, ranks)

    def attend_spatial(f, chunk):
        ones = jnp.ones((3 * span, LANES), BF)

        def pair_step(i, carry):
            for u in range(UNROLL):
                at = pl.ds(pl.multiple_of((UNROLL * i + u) * LANES, LANES), LANES)
                q = pr[0, f, 1 + chunk, :, :, at].reshape(span, LANES) * BF(SCALE)
                both = jnp.concatenate([q * masks[0], q * masks[1]], axis=0)
                k = pr[1, f, chunk:chunk + 3, :, :, at].reshape(3 * span, LANES)
                v = pr[2, f, chunk:chunk + 3, :, :, at].reshape(3 * span, LANES)
                sc = lax.dot_general(both, k, (((1,), (1,)), ((), ())), preferred_element_type=F32)
                sc = sc + jnp.concatenate([bias[f, chunk], bias[f, chunk]], axis=0)
                p = jnp.exp(sc - jnp.max(sc, axis=-1, keepdims=True)).astype(BF)
                o = jnp.dot(p, jnp.concatenate([v, ones], axis=1), preferred_element_type=F32)
                o = jnp.where(jnp.concatenate([lane, lane], axis=1) % LANES < HEAD_DIM, o[:span], o[span:])
                ctx1[:, at] = (o[:, :LANES] / o[:, LANES:]).astype(BF)
            return carry

        lax.fori_loop(0, depth // LANES // UNROLL, pair_step, 0)

    m_copies = {}

    def merge_spatial(f, chunk):
        def step(i, carry):
            at = pl.ds(pl.multiple_of(i * TILE, TILE), TILE)
            got = jnp.dot(ctx1[...], o1[:, at], preferred_element_type=F32)
            for source in range(ranks):
                base = source * blk
                total = got[base:base + blk] + xx[f, 1 + chunk, source, :, at].astype(F32)
                mid[(source - t) % ranks, f, chunk, :, at] = total.astype(BF)
            return carry

        lax.fori_loop(0, depth // TILE, step, 0)
        for j in away:
            copy = remote(mid.at[j, f, chunk], mids.at[j - 1, f, chunk], s_ms.at[f, chunk, j - 1],
                          s_mr.at[f, chunk, j - 1], "tm", (t + j) % ranks)
            copy.start()
            m_copies[f, chunk, j] = copy

    ready("w10", "w11", "w12")
    project_spatial([(f, slot, t) for f in range(frames) for slot in own], 0)
    for chunk in range(chunks - 1):
        forward(0, chunk)
    wait_halo(0, 0)
    project_spatial([(0, slot, t) for slot in ends], 1)
    forward(0, chunks - 1)
    project_spatial([(0, slot, (t - j) % ranks) for j in away for slot in own], 0)
    ready("o1")
    for f in range(frames):
        if f == 0:
            for j in away:
                wait_halo(f, j, (True,))
            project_spatial([(f, chunks + 1, (t - j) % ranks) for j in away], 1)
        else:
            for j in range(ranks):
                wait_halo(f, j)
            project_spatial([(f, slot, (t - j) % ranks) for j in range(ranks) for slot in ends], 1)
        if f + 1 < frames:
            for chunk in range(chunks - 1):
                forward(f + 1, chunk)
        for chunk in reversed(range(chunks)):
            if f == 0 and chunk == 0:
                for j in away:
                    wait_halo(f, j, (False,))
                project_spatial([(f, 0, (t - j) % ranks) for j in away], 1)
            attend_spatial(f, chunk)
            merge_spatial(f, chunk)
            if f + 1 < frames and chunk == chunks - 1:
                forward(f + 1, chunks - 1)
        if f + 1 < frames:
            project_spatial([(f + 1, slot, (t - j) % ranks) for j in away for slot in own], 0)

    for chunk in order[-1:]:
        send_cotangent(chunk, range(1, ranks))
    head = lax.broadcasted_iota(jnp.int32, (depth, LANES), 0) // HEAD_DIM
    gather[...] = (head == lax.broadcasted_iota(jnp.int32, (depth, LANES), 1)).astype(F32).astype(BF)
    head = lax.broadcasted_iota(jnp.int32, (LANES, depth), 1) // HEAD_DIM
    spread[...] = (head == lax.broadcasted_iota(jnp.int32, (LANES, depth), 0)).astype(F32).astype(BF)

    def project_temporal(blocks):
        for i, (j, f, chunk) in enumerate(blocks):
            value = mid[0, f, chunk] if j == 0 else mids[j - 1, f, chunk]
            nb[i * blk:(i + 1) * blk] = normalize(value, gain_two)
        count = len(blocks) * blk
        per = depth // TILE

        def step(i, carry):
            at = pl.ds(pl.multiple_of(i * TILE, TILE), TILE)
            lanes = pl.ds(pl.multiple_of(i % per * TILE, TILE), TILE)
            got = jnp.dot(nb[:count], w2[:, at], preferred_element_type=F32).astype(BF)
            for k, (j, f, chunk) in enumerate(blocks):
                qkv[i // per, chunk, j * frames + f, :, lanes] = got[k * blk:(k + 1) * blk]
            return carry

        lax.fori_loop(0, 3 * per, step, 0, unroll=True)

    ready("w2")
    project_temporal([(0, f, chunk) for f in range(frames) for chunk in range(chunks)])
    for f in range(frames):
        for j in away:
            for chunk in range(chunks):
                m_copies[f, chunk, j].wait_recv()
        project_temporal([(j, f, chunk) for j in away for chunk in range(chunks)])

    def frame_rank(slot):
        return order_ref[(t - slot // frames) % ranks * frames + slot % frames]

    k_order = [frame_rank(g) for g in range(keys)]

    def attend_temporal(chunk):
        def step(f, carry):
            q = qkv[0, chunk, f] * BF(SCALE)
            products = jnp.concatenate([q * qkv[1, chunk, g] for g in range(keys)], axis=0)
            scores = jnp.dot(products, gather[...], preferred_element_type=F32)
            own_order = frame_rank(f)
            kept = [scores[g * blk:(g + 1) * blk] + jnp.where(k_order[g] <= own_order, 0.0, -1e30)
                    for g in range(keys)]
            top_score = functools.reduce(jnp.maximum, kept)
            exps = [jnp.exp(sc - top_score) for sc in kept]
            scale = 1.0 / functools.reduce(jnp.add, exps)
            weights = jnp.concatenate([(e * scale).astype(BF) for e in exps], axis=0)
            spreads = jnp.dot(weights, spread[...], preferred_element_type=F32)
            total = None
            for g in range(keys):
                term = spreads[g * blk:(g + 1) * blk] * qkv[2, chunk, g].astype(F32)
                total = term if total is None else total + term
            ctx2[0, chunk, f] = total.astype(BF)
            return carry

        lax.fori_loop(0, keys, step, 0, unroll=4)

    row_tile = 1024
    sub = depth // (ranks * places * ny)
    stacked = keys * blk

    def add_gradient(terms, first, final):
        def step(i, carry):
            at = pl.ds(pl.multiple_of(i * row_tile, row_tile), row_tile)
            left = jnp.concatenate([ctx2[w, c, :, :, at].reshape(stacked, row_tile) for w, c in terms], axis=0)
            right = jnp.concatenate([cot[w, c].reshape(stacked, half) for w, c in terms], axis=0)
            got = lax.dot_general(left, right, (((0,), (0,)), ((), ())), preferred_element_type=F32)
            if not first:
                got = got + accf[at]
            if final:
                acc[at] = got.astype(BF)
            else:
                accf[at] = got
            return carry

        lax.fori_loop(0, depth // row_tile, step, 0)

    c_copies = {}
    ready(*[f"cot{f}" for f in range(frames)])
    before = None
    for chunk in order:
        attend_temporal(chunk)
        c_copies[chunk] = remote(ctx2.at[0, chunk], ctx2.at[1, chunk], s_cs.at[chunk], s_cr.at[chunk],
                                 "batch", other_core)
        c_copies[chunk].start()
        for of, copy in cot_copies:
            if of == chunk:
                copy.wait_recv()
        if before is not None:
            c_copies[before].wait_recv()
        add_gradient([(0, chunk)] + ([(1, before)] if before is not None else []), before is None, False)
        before = chunk
    c_copies[before].wait_recv()
    add_gradient([(1, before)], chunks == 0, True)

    sems = iter(range(s_gs.shape[0]))

    def exchange(axis, me, count, to_device, source, dests):
        copies = []
        for k in range(1, count):
            to = (me + k) % count
            n = next(sems)
            copy = remote(source(to), dests.at[k - 1], s_gs.at[n], s_gr.at[n], axis, to_device(to))
            copy.start()
            copies.append(copy)
        return copies

    def over_x(source, dests):
        return exchange("tm", t, ranks, lambda to: to, source, dests)

    def over_y(source, dests):
        return exchange("batch", y, ny, lambda to: to * 2 + core, source, dests)

    def over_z(source, dests):
        return exchange("space", s, places, lambda to: to, source, dests)

    def wait(copies):
        for copy in copies:
            copy.wait()

    def total_of(first, received, count):
        total = first.astype(F32)
        for k in range(count - 1):
            total = total + received[k].astype(F32)
        return total

    stage_one = []
    grid = acc.reshape(ranks, places, ny, sub, half)
    column = lambda n: slice(n * LANES, (n + 1) * LANES)
    count = half // LANES
    for n in range(count):
        if n % 2 == 0:
            stage_one.append(over_x(lambda to, n=n: grid.at[to, :, :, :, column(n)], xr_one.at[n // 2]))
        else:
            stage_one.append(over_y(lambda to, n=n: grid.at[:, :, to, :, column(n)], yr_one.at[n // 2]))

    ready("o2")

    def out_step(i, carry):
        at = pl.ds(pl.multiple_of(i * TILE, TILE), TILE)
        got = jnp.dot(ctx2[0].reshape(chunks * stacked, depth), o2[:, at], preferred_element_type=F32)
        for chunk in range(chunks):
            for j in range(ranks):
                for f in range(frames):
                    base = (chunk * keys + j * frames + f) * blk
                    value = mid[0, f, chunk, :, at] if j == 0 else mids[j - 1, f, chunk, :, at]
                    value = (value.astype(F32) + got[base:base + blk]).astype(BF)
                    if j == 0:
                        out[f, chunk, :, t, :, at] = value.reshape(inner + (TILE,))
                    else:
                        sent[(j - 1, chunk, f) + every + (at,)] = value.reshape(inner + (TILE,))
        return carry

    lax.fori_loop(0, depth // TILE, out_step, 0)
    out_copies = []

    def return_output():
        for chunk in range(chunks):
            for j in away:
                copy = remote(sent.at[j - 1, chunk], out.at[:, chunk, :, t], s_os.at[chunk, j - 1],
                              s_or.at[chunk, j - 1], "tm", (t - j) % ranks)
                copy.start()
                out_copies.append(copy)

    stage_two = []
    for n in range(count):
        wait(stage_one[n])
        k = n // 2
        if n % 2 == 0:
            one_x[k] = total_of(grid[t, :, :, :, column(n)], xr_one.at[k], ranks).astype(BF)
            stage_two.append(over_y(lambda to, k=k: one_x.at[k, :, to], yr_two.at[k]))
        else:
            one_y[k] = total_of(grid[:, :, y, :, column(n)], yr_one.at[k], ny).astype(BF)
            stage_two.append(over_x(lambda to, k=k: one_y.at[k, to], xr_two.at[k]))
    return_output()
    stage_three = []
    for n in range(count):
        wait(stage_two[n])
        k = n // 2
        if n % 2 == 0:
            two[n] = total_of(one_x[k, :, y], yr_two.at[k], ny).astype(BF)
        else:
            two[n] = total_of(one_y[k, t], xr_two.at[k], ranks).astype(BF)
        stage_three.append(over_z(lambda to, n=n: two.at[n, to], zr.at[n]))

    def place_piece(n, owner, value):
        rows_at = pl.ds(pl.multiple_of(owner // 2 * sub, sub), sub)
        lanes = pl.ds(pl.multiple_of(owner % 2 * half + n * LANES, LANES), LANES)
        grad[rows_at, lanes] = value.astype(F32)

    last = []
    for n in range(count):
        wait(stage_three[n])
        gp[n] = total_of(two[n, s], zr.at[n], places).astype(BF)
        last.append(exchange("batch", b, parts, lambda to: to, lambda to, n=n: gp.at[n], gr.at[n]))
        place_piece(n, b, gp[n])
    for n in range(count):
        for k, copy in enumerate(last[n]):
            copy.wait()
            place_piece(n, (b - 1 - k) % parts, gr[n, k])

    for copy in out_copies:
        copy.wait_recv()
    for copies in (x_copies, m_copies, c_copies):
        for copy in copies.values():
            copy.wait_send()
    for _, copy in cot_copies:
        copy.wait_send()
    for copy in out_copies:
        copy.wait_send()
    for f in range(frames):
        for j in range(ranks):
            finish_halo(f, j)


def per_device(clip_tokens, frame_order, row_reach, spatial_gain, spatial_heads, spatial_merge,
               temporal_gain, temporal_heads, temporal_merge, cotangent):
    ranks, places, parts = lax.axis_size("tm"), lax.axis_size("space"), lax.axis_size("batch")
    _, all_frames, rows, pc, depth = clip_tokens.shape
    frames, cols = all_frames // ranks, pc * ranks
    chunks, blk = rows // HALO, HALO * pc
    span = blk * ranks
    keys = ranks * frames
    ny = parts // 2
    half = depth // 2
    sub = depth // (ranks * places * ny)
    chunks_of = half // LANES
    pairs = chunks_of // 2
    inner = (HALO, pc) if pc % 16 == 0 else (1, blk)
    dims = (ranks, places, parts, frames, chunks, pc, depth, inner)
    anywhere = pl.BlockSpec(memory_space=pl.ANY)
    smem = pl.BlockSpec(memory_space=pltpu.SMEM)
    vmem = pl.BlockSpec(memory_space=pltpu.VMEM)
    dma = pltpu.SemaphoreType.DMA
    others, ny_others = max(ranks - 1, 1), max(ny - 1, 1)
    most = max(frames * chunks * blk, 2 * ranks * blk, (ranks - 1) * max(chunks, 2) * blk,
               (ranks - 1) * chunks * blk)
    steps = pairs * 2 * (ranks - 1) + pairs * 2 * (ny - 1) + chunks_of * (places - 1) + chunks_of * (parts - 1)
    scratch = [
        pltpu.VMEM((frames, chunks + 2, ranks, blk, depth), BF),
        pltpu.VMEM((others, frames, chunks, blk, depth), BF),
        pltpu.VMEM((3, frames, chunks + 2, ranks, blk, depth), BF),
        pltpu.VMEM((most, depth), BF),
        pltpu.VMEM((depth, 3 * depth), BF),
        pltpu.VMEM((depth, depth), BF),
        pltpu.VMEM((depth, 3 * depth), BF),
        pltpu.VMEM((depth, depth), BF),
        pltpu.VMEM((span, depth), BF),
        pltpu.VMEM((ranks, frames, chunks, blk, depth), BF),
        pltpu.VMEM((others, frames, chunks, blk, depth), BF),
        pltpu.VMEM((3, chunks, keys, blk, depth), BF),
        pltpu.VMEM((2, chunks, keys, blk, depth), BF),
        pltpu.VMEM((2, chunks, keys) + inner + (half,), BF),
        pltpu.VMEM((depth, LANES), BF),
        pltpu.VMEM((LANES, depth), BF),
        pltpu.VMEM((frames, chunks, span, 3 * span), F32),
        pltpu.VMEM((depth, half), F32),
        pltpu.VMEM((depth, half), BF),
        pltpu.VMEM((pairs, others, places, ny, sub, LANES), BF),
        pltpu.VMEM((pairs, ny_others, ranks, places, sub, LANES), BF),
        pltpu.VMEM((pairs, places, ny, sub, LANES), BF),
        pltpu.VMEM((pairs, ranks, places, sub, LANES), BF),
        pltpu.VMEM((pairs, others, places, sub, LANES), BF),
        pltpu.VMEM((pairs, ny_others, places, sub, LANES), BF),
        pltpu.VMEM((chunks_of, places, sub, LANES), BF),
        pltpu.VMEM((chunks_of, max(places - 1, 1), sub, LANES), BF),
        pltpu.VMEM((chunks_of, sub, LANES), BF),
        pltpu.VMEM((chunks_of, parts - 1, sub, LANES), BF),
        pltpu.VMEM((others, chunks, frames) + inner + (depth,), BF),
        dma((2 * frames + 6 + (ranks - 1) * frames,)),
        dma((frames, chunks, others)), dma((frames, chunks, others)),
        dma((2, frames, ranks)), dma((2, frames, ranks)),
        dma((frames, chunks, others)), dma((frames, chunks, others)),
        dma((2, chunks, ranks)), dma((2, chunks, ranks)),
        dma((chunks,)), dma((chunks,)),
        dma((chunks, others)), dma((chunks, others)),
        dma((steps,)), dma((steps,)),
    ]
    by_columns = cotangent.reshape(frames, chunks, HALO, ranks, pc, depth)
    if inner[0] == 1:
        by_columns = by_columns.transpose(0, 1, 3, 2, 4, 5).reshape(frames, chunks, 1, ranks, blk, depth)
    out, grad = pl.pallas_call(
        functools.partial(block_kernel, dims),
        out_shape=(pltpu.VMEM((frames, chunks, inner[0], ranks, inner[1], depth), BF),
                   pltpu.VMEM((ny * sub, depth), F32)),
        in_specs=[anywhere, smem, smem, vmem, vmem] + [anywhere] * 5,
        out_specs=(vmem, vmem),
        scratch_shapes=scratch,
        compiler_params=pltpu.CompilerParams(collective_id=0, has_side_effects=True,
                                             vmem_limit_bytes=60 << 20),
        name="block",
    )(clip_tokens.reshape(all_frames, chunks, blk, depth), frame_order.reshape(-1), row_reach.reshape(-1),
      spatial_gain.reshape(1, depth), temporal_gain.reshape(1, depth),
      spatial_heads, spatial_merge, temporal_heads, temporal_merge, by_columns)
    if inner[0] == 1:
        out = out.reshape(frames, chunks, ranks, HALO, pc, depth).transpose(0, 1, 3, 2, 4, 5)
    return out.reshape(1, frames, rows, cols, depth), grad


def solution(mesh):
    in_specs = (
        P("batch", None, "space", "tm", None),
        P("batch", None),
        P("batch", "tm"),
        P(),
        P(),
        P(),
        P(),
        P(),
        P(),
        P("batch", "tm", "space", None, None),
    )
    out_specs = (P("batch", "tm", "space", None, None), P(("tm", "space"), None))
    return jax.shard_map(per_device, mesh=mesh, in_specs=in_specs, out_specs=out_specs, check_vma=False)
```

```python
import functools

import jax
import jax.numpy as jnp
from jax import lax
from jax.experimental import pallas as pl
from jax.experimental.pallas import tpu as pltpu
from jax.sharding import PartitionSpec as P

HALO = 4
HEADS = 16
HEAD_DIM = 64
LANES = 128
TILE = 1024
UNROLL = 8
ROUTES = ("xyz", "yxz", "zxy", "yxz")
WAITS = ((0, 0), (1, 0), (3, 0), (1, 1), (0, 1), (2, 0), (3, 1), (2, 1), (0, 2), (1, 2), (2, 2), (3, 2))
SCALE = HEAD_DIM ** (-0.5)
FLOOR = 0.5
BF = jnp.bfloat16
F32 = jnp.float32
MESH = pl.DeviceIdType.MESH


def block_kernel(dims, *refs):
    ranks, places, parts, frames, chunks, pc, depth, inner = dims
    every = (slice(None), slice(None))
    (clip, order_ref, reach_ref, gain_one, gain_two, w_one, m_one, w_two, m_two, cot_in,
     out, grad,
     xx, away_x, pr, nb, w1, o1, w2, o2, ctx1, mid, mids, qkv, ctx2, cot, gather, spread, bias, accf, acc,
     gr, sent, *rest) = refs
    arrived, summed = rest[:3 * len(ROUTES)], rest[3 * len(ROUTES):6 * len(ROUTES)]
    (s_load, s_xs, s_xr, s_zs, s_zr, s_ms, s_mr, s_ts, s_tr, s_cs, s_cr, s_os, s_or, s_gs, s_gr) = rest[6 * len(ROUTES):]
    blk = HALO * pc
    span = blk * ranks
    rows = chunks * HALO
    keys = ranks * frames
    half = depth // 2
    t, s, b = lax.axis_index("tm"), lax.axis_index("space"), lax.axis_index("batch")
    core, y = b % 2, b // 2
    ny = parts // 2

    loads = {}

    def load(name, src, dst):
        copy = pltpu.make_async_copy(src, dst, s_load.at[len(loads)])
        copy.start()
        loads[name] = copy

    def ready(*names):
        for name in names:
            loads[name].wait()

    def half_of(which):
        return pl.ds(pl.multiple_of(which * half, half), half)

    for f in range(frames):
        load(f"x{f}", clip.at[t * frames + f], xx.at[f, 1:chunks + 1, t])
        for j in range(1, ranks):
            load(f"y{f}{j}", clip.at[(t + j) % ranks * frames + f], away_x.at[j - 1, f])
    for part in range(3):
        load(f"w1{part}", w_one.at[:, part * depth:(part + 1) * depth], w1.at[:, part * depth:(part + 1) * depth])
    load("o1", m_one, o1)
    load("w2", w_two, w2)
    load("o2", m_two, o2)
    for f in range(frames):
        load(f"cot{f}", cot_in.at[f, :, :, t, :, half_of(core)], cot.at[0, :, f])

    barrier = pltpu.get_barrier_semaphore()
    for axis, me, count in (("tm", t, ranks), ("space", s, places), ("batch", b, parts)):
        for shift in range(1, count):
            pl.semaphore_signal(barrier, inc=1, device_id={axis: (me + shift) % count}, device_id_type=MESH)
    other_core = b + 1 - 2 * core
    for j in range(1, ranks):
        pl.semaphore_signal(barrier, inc=1, device_id={"tm": (t + j) % ranks, "batch": other_core},
                            device_id_type=MESH)
    pl.semaphore_wait(barrier, 2 * ranks + places + parts - 4)

    ready(*[f"x{f}" for f in range(frames)], *[f"y{f}{j}" for f in range(frames) for j in range(1, ranks)])
    def remote(src, dst, send, recv, axis, to):
        return pltpu.make_async_remote_copy(src, dst, send, recv, device_id={axis: to}, device_id_type=MESH)

    x_copies = {}
    for f in range(frames):
        for chunk in range(chunks):
            for j in range(1, ranks):
                to = (t + j) % ranks
                copy = remote(away_x.at[j - 1, f, chunk], xx.at[f, 1 + chunk, t],
                              s_xs.at[f, chunk, j - 1], s_xr.at[f, chunk, j - 1], "tm", to)
                copy.start()
                x_copies[f, chunk, j] = copy

    def halo(f, j, up):
        source = (t - j) % ranks
        slot, dest = (1, chunks + 1) if up else (chunks, 0)
        return remote(xx.at[f, slot, source], xx.at[f, dest, source], s_zs.at[int(up), f, j], s_zr.at[int(up), f, j],
                      "space", (s - 1) if up else (s + 1))

    def send_halo(f, j, up):
        @pl.when((s > 0) if up else (s < places - 1))
        def _():
            halo(f, j, up).start()

    def wait_halo(f, j, sides=(False, True)):
        for up in sides:
            @pl.when((s < places - 1) if up else (s > 0))
            def _():
                halo(f, j, up).wait_recv()

    def finish_halo(f, j):
        @pl.when(s > 0)
        def _():
            halo(f, j, True).wait_send()

        @pl.when(s < places - 1)
        def _():
            halo(f, j, False).wait_send()

    def forward(f, chunk):
        for j in range(1, ranks):
            x_copies[f, chunk, j].wait_recv()
            if chunk == 0:
                send_halo(f, j, True)
            if chunk == chunks - 1:
                send_halo(f, j, False)
        if f + 1 < frames and chunk == 0:
            send_halo(f + 1, 0, True)
        if f + 1 < frames and chunk == chunks - 1:
            send_halo(f + 1, 0, False)

    send_halo(0, 0, True)
    send_halo(0, 0, False)
    cot_copies = []

    def send_cotangent(chunk, shifts):
        for j in shifts:
            to = (t + j) % ranks
            for which, core_to in ((0, core), (1, 1 - core)):
                if j == 0 and which == 0:
                    continue
                copy = pltpu.make_async_remote_copy(
                    cot_in.at[:, chunk, :, to, :, half_of(core_to)],
                    cot.at[which, chunk, j * frames:(j + 1) * frames],
                    s_ts.at[which, chunk, j], s_tr.at[which, chunk, j],
                    device_id={"tm": to, "batch": b - core + core_to}, device_id_type=MESH)
                copy.start()
                cot_copies.append((chunk, copy))

    order = list(reversed(range(chunks)))
    for chunk in order:
        send_cotangent(chunk, range(1))
    for chunk in order[:-1]:
        send_cotangent(chunk, range(1, ranks))

    @pl.when(s == 0)
    def _():
        xx[:, 0] = jnp.zeros((frames, ranks, blk, depth), BF)

    @pl.when(s == places - 1)
    def _():
        xx[:, chunks + 1] = jnp.zeros((frames, ranks, blk, depth), BF)

    lane = lax.broadcasted_iota(jnp.int32, (1, LANES), 1)
    first_head = (lane < HEAD_DIM).astype(F32)
    masks = (first_head.astype(BF), (1.0 - first_head).astype(BF))
    for f in range(frames):
        for chunk in range(chunks):
            shape = (span, 3 * span)
            q_row = chunk * HALO + lax.broadcasted_iota(jnp.int32, shape, 0) % blk // pc
            k_at = lax.broadcasted_iota(jnp.int32, shape, 1)
            k_row = (chunk - 1 + k_at // span) * HALO + k_at % blk // pc
            place = s * rows + k_row
            kept = (jnp.abs(k_row - q_row) <= reach_ref[f]) & (place >= 0) & (place < rows * places)
            bias[f, chunk] = jnp.where(kept, 0.0, -1e30)

    def normalize(values, gain):
        widened = values.astype(F32)
        scaled = widened * lax.rsqrt(jnp.mean(widened * widened, axis=-1, keepdims=True) + FLOOR)
        return (scaled * gain[...]).astype(BF)

    def project_spatial(blocks, first):
        for i, (f, slot, source) in enumerate(blocks):
            nb[i * blk:(i + 1) * blk] = normalize(xx[f, slot, source], gain_one)
        count = len(blocks) * blk
        per = depth // TILE

        def step(i, carry):
            at = pl.ds(pl.multiple_of(i * TILE, TILE), TILE)
            lanes = pl.ds(pl.multiple_of(i % per * TILE, TILE), TILE)
            got = jnp.dot(nb[:count], w1[:, at], preferred_element_type=F32).astype(BF)
            for k, (f, slot, source) in enumerate(blocks):
                pr[i // per, f, slot, source, :, lanes] = got[k * blk:(k + 1) * blk]
            return carry

        lax.fori_loop(first * per, 3 * per, step, 0, unroll=True)

    own = range(1, chunks + 1)
    ends = (0, chunks + 1)
    away = range(1, ranks)

    def attend_spatial(f, chunk):
        ones = jnp.ones((3 * span, LANES), BF)

        def pair_step(i, carry):
            for u in range(UNROLL):
                at = pl.ds(pl.multiple_of((UNROLL * i + u) * LANES, LANES), LANES)
                q = pr[0, f, 1 + chunk, :, :, at].reshape(span, LANES) * BF(SCALE)
                both = jnp.concatenate([q * masks[0], q * masks[1]], axis=0)
                k = pr[1, f, chunk:chunk + 3, :, :, at].reshape(3 * span, LANES)
                v = pr[2, f, chunk:chunk + 3, :, :, at].reshape(3 * span, LANES)
                sc = lax.dot_general(both, k, (((1,), (1,)), ((), ())), preferred_element_type=F32)
                sc = sc + jnp.concatenate([bias[f, chunk], bias[f, chunk]], axis=0)
                p = jnp.exp(sc - jnp.max(sc, axis=-1, keepdims=True)).astype(BF)
                o = jnp.dot(p, jnp.concatenate([v, ones], axis=1), preferred_element_type=F32)
                o = jnp.where(jnp.concatenate([lane, lane], axis=1) % LANES < HEAD_DIM, o[:span], o[span:])
                ctx1[:, at] = (o[:, :LANES] / o[:, LANES:]).astype(BF)
            return carry

        lax.fori_loop(0, depth // LANES // UNROLL, pair_step, 0)

    m_copies = {}

    def merge_spatial(f, chunk):
        def step(i, carry):
            at = pl.ds(pl.multiple_of(i * TILE, TILE), TILE)
            got = jnp.dot(ctx1[...], o1[:, at], preferred_element_type=F32)
            for source in range(ranks):
                base = source * blk
                total = got[base:base + blk] + xx[f, 1 + chunk, source, :, at].astype(F32)
                mid[(source - t) % ranks, f, chunk, :, at] = total.astype(BF)
            return carry

        lax.fori_loop(0, depth // TILE, step, 0)
        for j in away:
            copy = remote(mid.at[j, f, chunk], mids.at[j - 1, f, chunk], s_ms.at[f, chunk, j - 1],
                          s_mr.at[f, chunk, j - 1], "tm", (t + j) % ranks)
            copy.start()
            m_copies[f, chunk, j] = copy

    ready("w10", "w11", "w12")
    project_spatial([(f, slot, t) for f in range(frames) for slot in own], 0)
    for chunk in range(chunks - 1):
        forward(0, chunk)
    wait_halo(0, 0)
    project_spatial([(0, slot, t) for slot in ends], 1)
    forward(0, chunks - 1)
    project_spatial([(0, slot, (t - j) % ranks) for j in away for slot in own], 0)
    ready("o1")
    for f in range(frames):
        if f == 0:
            for j in away:
                wait_halo(f, j, (True,))
            project_spatial([(f, chunks + 1, (t - j) % ranks) for j in away], 1)
        else:
            for j in range(ranks):
                wait_halo(f, j)
            project_spatial([(f, slot, (t - j) % ranks) for j in range(ranks) for slot in ends], 1)
        if f + 1 < frames:
            for chunk in range(chunks - 1):
                forward(f + 1, chunk)
        for chunk in reversed(range(chunks)):
            if f == 0 and chunk == 0:
                for j in away:
                    wait_halo(f, j, (False,))
                project_spatial([(f, 0, (t - j) % ranks) for j in away], 1)
            attend_spatial(f, chunk)
            merge_spatial(f, chunk)
            if f + 1 < frames and chunk == chunks - 1:
                forward(f + 1, chunks - 1)
        if f + 1 < frames:
            project_spatial([(f + 1, slot, (t - j) % ranks) for j in away for slot in own], 0)

    for chunk in order[-1:]:
        send_cotangent(chunk, range(1, ranks))
    head = lax.broadcasted_iota(jnp.int32, (depth, LANES), 0) // HEAD_DIM
    gather[...] = (head == lax.broadcasted_iota(jnp.int32, (depth, LANES), 1)).astype(F32).astype(BF)
    head = lax.broadcasted_iota(jnp.int32, (LANES, depth), 1) // HEAD_DIM
    spread[...] = (head == lax.broadcasted_iota(jnp.int32, (LANES, depth), 0)).astype(F32).astype(BF)

    def project_temporal(blocks):
        for i, (j, f, chunk) in enumerate(blocks):
            value = mid[0, f, chunk] if j == 0 else mids[j - 1, f, chunk]
            nb[i * blk:(i + 1) * blk] = normalize(value, gain_two)
        count = len(blocks) * blk
        per = depth // TILE

        def step(i, carry):
            at = pl.ds(pl.multiple_of(i * TILE, TILE), TILE)
            lanes = pl.ds(pl.multiple_of(i % per * TILE, TILE), TILE)
            got = jnp.dot(nb[:count], w2[:, at], preferred_element_type=F32).astype(BF)
            for k, (j, f, chunk) in enumerate(blocks):
                qkv[i // per, chunk, j * frames + f, :, lanes] = got[k * blk:(k + 1) * blk]
            return carry

        lax.fori_loop(0, 3 * per, step, 0, unroll=True)

    ready("w2")
    project_temporal([(0, f, chunk) for f in range(frames) for chunk in range(chunks)])
    final = frames - 1
    for f in range(final):
        for j in away:
            for chunk in range(chunks):
                m_copies[f, chunk, j].wait_recv()
        project_temporal([(j, f, chunk) for j in away for chunk in range(chunks)])

    def frame_rank(slot):
        return order_ref[(t - slot // frames) % ranks * frames + slot % frames]

    k_order = [frame_rank(g) for g in range(keys)]

    def attend_temporal(chunk):
        def step(f, carry):
            q = qkv[0, chunk, f] * BF(SCALE)
            products = jnp.concatenate([q * qkv[1, chunk, g] for g in range(keys)], axis=0)
            scores = jnp.dot(products, gather[...], preferred_element_type=F32)
            own_order = frame_rank(f)
            kept = [scores[g * blk:(g + 1) * blk] + jnp.where(k_order[g] <= own_order, 0.0, -1e30)
                    for g in range(keys)]
            top_score = functools.reduce(jnp.maximum, kept)
            exps = [jnp.exp(sc - top_score) for sc in kept]
            scale = 1.0 / functools.reduce(jnp.add, exps)
            weights = jnp.concatenate([(e * scale).astype(BF) for e in exps], axis=0)
            spreads = jnp.dot(weights, spread[...], preferred_element_type=F32)
            total = None
            for g in range(keys):
                term = spreads[g * blk:(g + 1) * blk] * qkv[2, chunk, g].astype(F32)
                total = term if total is None else total + term
            ctx2[0, chunk, f] = total.astype(BF)
            return carry

        lax.fori_loop(0, keys, step, 0, unroll=4)

    row_tile = 1024
    sub = depth // (ranks * places * ny)
    stacked = keys * blk

    def add_gradient(terms, first, final):
        def step(i, carry):
            at = pl.ds(pl.multiple_of(i * row_tile, row_tile), row_tile)
            left = jnp.concatenate([ctx2[w, c, :, :, at].reshape(stacked, row_tile) for w, c in terms], axis=0)
            right = jnp.concatenate([cot[w, c].reshape(stacked, half) for w, c in terms], axis=0)
            got = lax.dot_general(left, right, (((0,), (0,)), ((), ())), preferred_element_type=F32)
            if not first:
                got = got + accf[at]
            if final:
                acc[at] = got.astype(BF)
            else:
                accf[at] = got
            return carry

        lax.fori_loop(0, depth // row_tile, step, 0)

    def merge_temporal(chunk):
        got = jnp.dot(ctx2[0, chunk].reshape(stacked, depth), o2[...], preferred_element_type=F32)
        for j in range(ranks):
            for f in range(frames):
                base = (j * frames + f) * blk
                value = mid[0, f, chunk] if j == 0 else mids[j - 1, f, chunk]
                value = (value.astype(F32) + got[base:base + blk]).astype(BF).reshape(inner + (depth,))
                if j == 0:
                    out[f, chunk, :, t] = value
                else:
                    sent[j - 1, chunk, f] = value

    out_copies = []
    returns = {chunk: [(chunk, f, j) for f in range(frames) for j in away] for chunk in order}

    def return_output(some):
        for chunk, f, j in some:
            copy = remote(sent.at[j - 1, chunk, f], out.at[f, chunk, :, t], s_os.at[chunk, f, j - 1],
                          s_or.at[chunk, f, j - 1], "tm", (t - j) % ranks)
            copy.start()
            out_copies.append(copy)

    c_copies = {}
    ready(*[f"cot{f}" for f in range(frames)])
    ready("o2")
    before = None
    for chunk in order:
        for j in away:
            m_copies[final, chunk, j].wait_recv()
        project_temporal([(j, final, chunk) for j in away])
        attend_temporal(chunk)
        c_copies[chunk] = remote(ctx2.at[0, chunk], ctx2.at[1, chunk], s_cs.at[chunk], s_cr.at[chunk],
                                 "batch", other_core)
        c_copies[chunk].start()
        for of, copy in cot_copies:
            if of == chunk:
                copy.wait_recv()
        if before is not None:
            c_copies[before].wait_recv()
        add_gradient([(0, chunk)] + ([(1, before)] if before is not None else []), before is None, False)
        if chunk != order[-1]:
            merge_temporal(chunk)
            return_output(returns[chunk][:len(returns[chunk]) // 2])
        before = chunk
    c_copies[before].wait_recv()
    add_gradient([(1, before)], chunks == 0, True)

    sems = iter(range(s_gs.shape[0]))
    axes = {"x": ("tm", t, ranks, lambda to: to), "z": ("space", s, places, lambda to: to),
            "y": ("batch", y, ny, lambda to: to * 2 + core)}
    column = lambda n: slice(n * LANES, (n + 1) * LANES)
    count = half // LANES
    grid = acc.reshape(ranks, places, ny, sub, half)

    def exchange(axis, source, dests):
        name, me, size, device = axes[axis]
        copies = []
        for k in range(1, size):
            to = (me + k) % size
            n = next(sems)
            copy = remote(source(to), dests.at[k - 1], s_gs.at[n], s_gr.at[n], name, device(to))
            copy.start()
            copies.append(copy)
        return copies

    def place_in(n, stage, value):
        route = ROUTES[n]
        left = [a for a in "xzy" if a not in route[:stage]]
        at = tuple(value if a == route[stage] else slice(None) for a in left)
        return at + (slice(None), column(n)) if stage == 0 else at

    flying = {}

    def launch(n, stage):
        src = grid if stage == 0 else summed[3 * n + stage - 1]
        flying[n, stage] = exchange(ROUTES[n][stage], lambda to: src.at[place_in(n, stage, to)],
                                    arrived[3 * n + stage])

    def finish(n, stage):
        for copy in flying[n, stage]:
            copy.wait()
        src = grid if stage == 0 else summed[3 * n + stage - 1]
        _, me, size, _ = axes[ROUTES[n][stage]]
        total = src[place_in(n, stage, me)].astype(F32)
        for k in range(size - 1):
            total = total + arrived[3 * n + stage][k].astype(F32)
        summed[3 * n + stage][...] = total.astype(BF)
        if stage < 2:
            launch(n, stage + 1)

    def place_piece(n, owner, value):
        rows_at = pl.ds(pl.multiple_of(owner // 2 * sub, sub), sub)
        lanes = pl.ds(pl.multiple_of(owner % 2 * half + n * LANES, LANES), LANES)
        grad[rows_at, lanes] = value.astype(F32)

    last = {}

    def gather_piece(n):
        piece = summed[3 * n + 2]
        last[n] = []
        for k in range(1, parts):
            at = next(sems)
            copy = remote(piece, gr.at[n, k - 1], s_gs.at[at], s_gr.at[at], "batch", (b + k) % parts)
            copy.start()
            last[n].append(copy)
        place_piece(n, b, piece[...])

    for n in range(count):
        launch(n, 0)

    for chunk in order[:-1]:
        return_output(returns[chunk][len(returns[chunk]) // 2:])
    merge_temporal(order[-1])
    for n, stage in WAITS:
        finish(n, stage)
        if (n, stage) == (2, 0):
            return_output(returns[order[-1]])
        if stage == 2:
            gather_piece(n)
    for n in last:
        for k, copy in enumerate(last[n]):
            copy.wait()
            place_piece(n, (b - 1 - k) % parts, gr[n, k])

    for copy in out_copies:
        copy.wait_recv()
    for copies in (x_copies, m_copies, c_copies):
        for copy in copies.values():
            copy.wait_send()
    for _, copy in cot_copies:
        copy.wait_send()
    for copy in out_copies:
        copy.wait_send()
    for f in range(frames):
        for j in range(ranks):
            finish_halo(f, j)


def per_device(clip_tokens, frame_order, row_reach, spatial_gain, spatial_heads, spatial_merge,
               temporal_gain, temporal_heads, temporal_merge, cotangent):
    ranks, places, parts = lax.axis_size("tm"), lax.axis_size("space"), lax.axis_size("batch")
    _, all_frames, rows, pc, depth = clip_tokens.shape
    frames, cols = all_frames // ranks, pc * ranks
    chunks, blk = rows // HALO, HALO * pc
    span = blk * ranks
    keys = ranks * frames
    ny = parts // 2
    half = depth // 2
    sub = depth // (ranks * places * ny)
    chunks_of = half // LANES
    inner = (HALO, pc) if pc % 16 == 0 else (1, blk)
    dims = (ranks, places, parts, frames, chunks, pc, depth, inner)
    anywhere = pl.BlockSpec(memory_space=pl.ANY)
    smem = pl.BlockSpec(memory_space=pltpu.SMEM)
    vmem = pl.BlockSpec(memory_space=pltpu.VMEM)
    dma = pltpu.SemaphoreType.DMA
    others = max(ranks - 1, 1)
    most = max(frames * chunks * blk, 2 * ranks * blk, (ranks - 1) * max(chunks, 2) * blk,
               (ranks - 1) * chunks * blk)
    sizes = {"x": ranks, "z": places, "y": ny}
    arrivals, sums, steps = [], [], 0
    for route in ROUTES:
        for stage in range(3):
            left = tuple(sizes[a] for a in "xzy" if a not in route[:stage + 1])
            arrivals.append(pltpu.VMEM((max(sizes[route[stage]] - 1, 1),) + left + (sub, LANES), BF))
            sums.append(pltpu.VMEM(left + (sub, LANES), BF))
            steps += sizes[route[stage]] - 1
        steps += parts - 1
    scratch = [
        pltpu.VMEM((frames, chunks + 2, ranks, blk, depth), BF),
        pltpu.VMEM((others, frames, chunks, blk, depth), BF),
        pltpu.VMEM((3, frames, chunks + 2, ranks, blk, depth), BF),
        pltpu.VMEM((most, depth), BF),
        pltpu.VMEM((depth, 3 * depth), BF),
        pltpu.VMEM((depth, depth), BF),
        pltpu.VMEM((depth, 3 * depth), BF),
        pltpu.VMEM((depth, depth), BF),
        pltpu.VMEM((span, depth), BF),
        pltpu.VMEM((ranks, frames, chunks, blk, depth), BF),
        pltpu.VMEM((others, frames, chunks, blk, depth), BF),
        pltpu.VMEM((3, chunks, keys, blk, depth), BF),
        pltpu.VMEM((2, chunks, keys, blk, depth), BF),
        pltpu.VMEM((2, chunks, keys) + inner + (half,), BF),
        pltpu.VMEM((depth, LANES), BF),
        pltpu.VMEM((LANES, depth), BF),
        pltpu.VMEM((frames, chunks, span, 3 * span), F32),
        pltpu.VMEM((depth, half), F32),
        pltpu.VMEM((depth, half), BF),
        pltpu.VMEM((chunks_of, parts - 1, sub, LANES), BF),
        pltpu.VMEM((others, chunks, frames) + inner + (depth,), BF),
        *arrivals, *sums,
        dma((2 * frames + 6 + (ranks - 1) * frames,)),
        dma((frames, chunks, others)), dma((frames, chunks, others)),
        dma((2, frames, ranks)), dma((2, frames, ranks)),
        dma((frames, chunks, others)), dma((frames, chunks, others)),
        dma((2, chunks, ranks)), dma((2, chunks, ranks)),
        dma((chunks,)), dma((chunks,)),
        dma((chunks, frames, others)), dma((chunks, frames, others)),
        dma((steps,)), dma((steps,)),
    ]
    by_columns = cotangent.reshape(frames, chunks, HALO, ranks, pc, depth)
    if inner[0] == 1:
        by_columns = by_columns.transpose(0, 1, 3, 2, 4, 5).reshape(frames, chunks, 1, ranks, blk, depth)
    out, grad = pl.pallas_call(
        functools.partial(block_kernel, dims),
        out_shape=(pltpu.VMEM((frames, chunks, inner[0], ranks, inner[1], depth), BF),
                   pltpu.VMEM((ny * sub, depth), F32)),
        in_specs=[anywhere, smem, smem, vmem, vmem] + [anywhere] * 5,
        out_specs=(vmem, vmem),
        scratch_shapes=scratch,
        compiler_params=pltpu.CompilerParams(collective_id=0, has_side_effects=True,
                                             vmem_limit_bytes=60 << 20),
        name="block",
    )(clip_tokens.reshape(all_frames, chunks, blk, depth), frame_order.reshape(-1), row_reach.reshape(-1),
      spatial_gain.reshape(1, depth), temporal_gain.reshape(1, depth),
      spatial_heads, spatial_merge, temporal_heads, temporal_merge, by_columns)
    if inner[0] == 1:
        out = out.reshape(frames, chunks, ranks, HALO, pc, depth).transpose(0, 1, 3, 2, 4, 5)
    return out.reshape(1, frames, rows, cols, depth), grad


def solution(mesh):
    in_specs = (
        P("batch", None, "space", "tm", None),
        P("batch", None),
        P("batch", "tm"),
        P(),
        P(),
        P(),
        P(),
        P(),
        P(),
        P("batch", "tm", "space", None, None),
    )
    out_specs = (P("batch", "tm", "space", None, None), P(("tm", "space"), None))
    return jax.shard_map(per_device, mesh=mesh, in_specs=in_specs, out_specs=out_specs, check_vma=False)
```

```python
import functools

import jax
import jax.numpy as jnp
from jax import lax
from jax.experimental import pallas as pl
from jax.experimental.pallas import tpu as pltpu
from jax.sharding import PartitionSpec as P

HALO = 4
HEADS = 16
HEAD_DIM = 64
LANES = 128
TILE = 1024
UNROLL = 8
ROUTES = ("xyz", "yxz", "zxy", "yxz")
WAITS = ((0, 0), (1, 0), (3, 0), (1, 1), (0, 1), (2, 0), (3, 1), (2, 1), (0, 2), (1, 2), (2, 2), (3, 2))
SCALE = HEAD_DIM ** (-0.5)
FLOOR = 0.5
BF = jnp.bfloat16
F32 = jnp.float32
MESH = pl.DeviceIdType.MESH


def block_kernel(dims, *refs):
    ranks, places, parts, frames, chunks, pc, depth, inner = dims
    every = (slice(None), slice(None))
    (clip, order_in, reach_in, gain_one_in, gain_two_in, w_one, m_one, w_two, m_two, cot_in,
     out, grad,
     xx, away_x, pr, nb, w1, o1, w2, o2, ctx1, mid, mids, qkv, ctx2, cot, gather, spread, bias, accf, acc,
     gr, sent, order_ref, reach_ref, gain_one, gain_two, *rest) = refs
    arrived, summed = rest[:3 * len(ROUTES)], rest[3 * len(ROUTES):6 * len(ROUTES)]
    (s_load, s_xs, s_xr, s_zs, s_zr, s_ms, s_mr, s_ts, s_tr, s_cs, s_cr, s_os, s_or, s_gs, s_gr) = rest[6 * len(ROUTES):]
    blk = HALO * pc
    span = blk * ranks
    rows = chunks * HALO
    keys = ranks * frames
    half = depth // 2
    t, s, b = lax.axis_index("tm"), lax.axis_index("space"), lax.axis_index("batch")
    core, y = b % 2, b // 2
    ny = parts // 2

    loads = {}

    def load(name, src, dst):
        copy = pltpu.make_async_copy(src, dst, s_load.at[len(loads)])
        copy.start()
        loads[name] = copy

    def ready(*names):
        for name in names:
            loads[name].wait()

    def half_of(which):
        return pl.ds(pl.multiple_of(which * half, half), half)

    for f in range(frames):
        load(f"x{f}", clip.at[t * frames + f], xx.at[f, 1:chunks + 1, t])
        for j in range(1, ranks):
            load(f"y{f}{j}", clip.at[(t + j) % ranks * frames + f], away_x.at[j - 1, f])
    for name, src, dst in (("reach", reach_in, reach_ref), ("order", order_in, order_ref),
                           ("gain1", gain_one_in, gain_one), ("gain2", gain_two_in, gain_two)):
        load(name, src, dst)
    for part in range(3):
        load(f"w1{part}", w_one.at[:, part * depth:(part + 1) * depth], w1.at[:, part * depth:(part + 1) * depth])
    load("o1", m_one, o1)
    load("w2", w_two, w2)
    load("o2", m_two, o2)
    for f in range(frames):
        load(f"cot{f}", cot_in.at[f, :, :, t, :, half_of(core)], cot.at[0, :, f])

    barrier = pltpu.get_barrier_semaphore()
    for axis, me, count in (("tm", t, ranks), ("space", s, places), ("batch", b, parts)):
        for shift in range(1, count):
            pl.semaphore_signal(barrier, inc=1, device_id={axis: (me + shift) % count}, device_id_type=MESH)
    other_core = b + 1 - 2 * core
    for j in range(1, ranks):
        pl.semaphore_signal(barrier, inc=1, device_id={"tm": (t + j) % ranks, "batch": other_core},
                            device_id_type=MESH)
    pl.semaphore_wait(barrier, 2 * ranks + places + parts - 4)

    ready(*[f"x{f}" for f in range(frames)], *[f"y{f}{j}" for f in range(frames) for j in range(1, ranks)])
    def remote(src, dst, send, recv, axis, to):
        return pltpu.make_async_remote_copy(src, dst, send, recv, device_id={axis: to}, device_id_type=MESH)

    x_copies = {}
    for f in range(frames):
        for chunk in range(chunks):
            for j in range(1, ranks):
                to = (t + j) % ranks
                copy = remote(away_x.at[j - 1, f, chunk], xx.at[f, 1 + chunk, t],
                              s_xs.at[f, chunk, j - 1], s_xr.at[f, chunk, j - 1], "tm", to)
                copy.start()
                x_copies[f, chunk, j] = copy

    def halo(f, j, up):
        source = (t - j) % ranks
        slot, dest = (1, chunks + 1) if up else (chunks, 0)
        return remote(xx.at[f, slot, source], xx.at[f, dest, source], s_zs.at[int(up), f, j], s_zr.at[int(up), f, j],
                      "space", (s - 1) if up else (s + 1))

    def send_halo(f, j, up):
        @pl.when((s > 0) if up else (s < places - 1))
        def _():
            halo(f, j, up).start()

    def wait_halo(f, j, sides=(False, True)):
        for up in sides:
            @pl.when((s < places - 1) if up else (s > 0))
            def _():
                halo(f, j, up).wait_recv()

    def finish_halo(f, j):
        @pl.when(s > 0)
        def _():
            halo(f, j, True).wait_send()

        @pl.when(s < places - 1)
        def _():
            halo(f, j, False).wait_send()

    def forward(f, chunk):
        for j in range(1, ranks):
            x_copies[f, chunk, j].wait_recv()
            if chunk == 0:
                send_halo(f, j, True)
            if chunk == chunks - 1:
                send_halo(f, j, False)
        if f + 1 < frames and chunk == 0:
            send_halo(f + 1, 0, True)
        if f + 1 < frames and chunk == chunks - 1:
            send_halo(f + 1, 0, False)

    send_halo(0, 0, True)
    send_halo(0, 0, False)
    cot_copies = []

    def send_cotangent(chunk, shifts):
        for j in shifts:
            to = (t + j) % ranks
            for which, core_to in ((0, core), (1, 1 - core)):
                if j == 0 and which == 0:
                    continue
                copy = pltpu.make_async_remote_copy(
                    cot_in.at[:, chunk, :, to, :, half_of(core_to)],
                    cot.at[which, chunk, j * frames:(j + 1) * frames],
                    s_ts.at[which, chunk, j], s_tr.at[which, chunk, j],
                    device_id={"tm": to, "batch": b - core + core_to}, device_id_type=MESH)
                copy.start()
                cot_copies.append((chunk, copy))

    order = list(reversed(range(chunks)))
    for chunk in order:
        send_cotangent(chunk, range(1))
    for chunk in order[:-1]:
        send_cotangent(chunk, range(1, ranks))

    @pl.when(s == 0)
    def _():
        xx[:, 0] = jnp.zeros((frames, ranks, blk, depth), BF)

    @pl.when(s == places - 1)
    def _():
        xx[:, chunks + 1] = jnp.zeros((frames, ranks, blk, depth), BF)

    ready("reach", "gain1")
    lane = lax.broadcasted_iota(jnp.int32, (1, LANES), 1)
    first_head = (lane < HEAD_DIM).astype(F32)
    masks = (first_head.astype(BF), (1.0 - first_head).astype(BF))
    for f in range(frames):
        for chunk in range(chunks):
            shape = (span, 3 * span)
            q_row = chunk * HALO + lax.broadcasted_iota(jnp.int32, shape, 0) % blk // pc
            k_at = lax.broadcasted_iota(jnp.int32, shape, 1)
            k_row = (chunk - 1 + k_at // span) * HALO + k_at % blk // pc
            place = s * rows + k_row
            kept = (jnp.abs(k_row - q_row) <= reach_ref[f]) & (place >= 0) & (place < rows * places)
            bias[f, chunk] = jnp.where(kept, 0.0, -1e30)

    def normalize(values, gain):
        widened = values.astype(F32)
        scaled = widened * lax.rsqrt(jnp.mean(widened * widened, axis=-1, keepdims=True) + FLOOR)
        return (scaled * gain[...]).astype(BF)

    def project_spatial(blocks, first):
        for i, (f, slot, source) in enumerate(blocks):
            nb[i * blk:(i + 1) * blk] = normalize(xx[f, slot, source], gain_one)
        count = len(blocks) * blk
        per = depth // TILE

        def step(i, carry):
            at = pl.ds(pl.multiple_of(i * TILE, TILE), TILE)
            lanes = pl.ds(pl.multiple_of(i % per * TILE, TILE), TILE)
            got = jnp.dot(nb[:count], w1[:, at], preferred_element_type=F32).astype(BF)
            for k, (f, slot, source) in enumerate(blocks):
                pr[i // per, f, slot, source, :, lanes] = got[k * blk:(k + 1) * blk]
            return carry

        lax.fori_loop(first * per, 3 * per, step, 0, unroll=True)

    own = range(1, chunks + 1)
    ends = (0, chunks + 1)
    away = range(1, ranks)

    def attend_spatial(f, chunk):
        ones = jnp.ones((3 * span, LANES), BF)

        def pair_step(i, carry):
            for u in range(UNROLL):
                at = pl.ds(pl.multiple_of((UNROLL * i + u) * LANES, LANES), LANES)
                q = pr[0, f, 1 + chunk, :, :, at].reshape(span, LANES) * BF(SCALE)
                both = jnp.concatenate([q * masks[0], q * masks[1]], axis=0)
                k = pr[1, f, chunk:chunk + 3, :, :, at].reshape(3 * span, LANES)
                v = pr[2, f, chunk:chunk + 3, :, :, at].reshape(3 * span, LANES)
                sc = lax.dot_general(both, k, (((1,), (1,)), ((), ())), preferred_element_type=F32)
                sc = sc + jnp.concatenate([bias[f, chunk], bias[f, chunk]], axis=0)
                p = jnp.exp(sc - jnp.max(sc, axis=-1, keepdims=True)).astype(BF)
                o = jnp.dot(p, jnp.concatenate([v, ones], axis=1), preferred_element_type=F32)
                o = jnp.where(jnp.concatenate([lane, lane], axis=1) % LANES < HEAD_DIM, o[:span], o[span:])
                ctx1[:, at] = (o[:, :LANES] / o[:, LANES:]).astype(BF)
            return carry

        lax.fori_loop(0, depth // LANES // UNROLL, pair_step, 0)

    m_copies = {}

    def merge_spatial(f, chunk):
        def step(i, carry):
            at = pl.ds(pl.multiple_of(i * TILE, TILE), TILE)
            got = jnp.dot(ctx1[...], o1[:, at], preferred_element_type=F32)
            for source in range(ranks):
                base = source * blk
                total = got[base:base + blk] + xx[f, 1 + chunk, source, :, at].astype(F32)
                mid[(source - t) % ranks, f, chunk, :, at] = total.astype(BF)
            return carry

        lax.fori_loop(0, depth // TILE, step, 0)
        for j in away:
            copy = remote(mid.at[j, f, chunk], mids.at[j - 1, f, chunk], s_ms.at[f, chunk, j - 1],
                          s_mr.at[f, chunk, j - 1], "tm", (t + j) % ranks)
            copy.start()
            m_copies[f, chunk, j] = copy

    ready("w10", "w11", "w12")
    project_spatial([(f, slot, t) for f in range(frames) for slot in own], 0)
    for chunk in range(chunks - 1):
        forward(0, chunk)
    wait_halo(0, 0)
    project_spatial([(0, slot, t) for slot in ends], 1)
    forward(0, chunks - 1)
    project_spatial([(0, slot, (t - j) % ranks) for j in away for slot in own], 0)
    ready("o1")
    for f in range(frames):
        if f == 0:
            for j in away:
                wait_halo(f, j, (True,))
            project_spatial([(f, chunks + 1, (t - j) % ranks) for j in away], 1)
        else:
            for j in range(ranks):
                wait_halo(f, j)
            project_spatial([(f, slot, (t - j) % ranks) for j in range(ranks) for slot in ends], 1)
        for chunk in reversed(range(chunks)):
            if f == 0 and chunk == 0:
                for j in away:
                    wait_halo(f, j, (False,))
                project_spatial([(f, 0, (t - j) % ranks) for j in away], 1)
            if f + 1 < frames and chunk == 0:
                forward(f + 1, chunks - 1)
            attend_spatial(f, chunk)
            if f + 1 < frames and chunk == chunks - 1:
                for early in range(chunks - 1):
                    forward(f + 1, early)
            merge_spatial(f, chunk)
        if f + 1 < frames:
            project_spatial([(f + 1, slot, (t - j) % ranks) for j in away for slot in own], 0)

    for chunk in order[-1:]:
        send_cotangent(chunk, range(1, ranks))
    head = lax.broadcasted_iota(jnp.int32, (depth, LANES), 0) // HEAD_DIM
    gather[...] = (head == lax.broadcasted_iota(jnp.int32, (depth, LANES), 1)).astype(F32).astype(BF)
    head = lax.broadcasted_iota(jnp.int32, (LANES, depth), 1) // HEAD_DIM
    spread[...] = (head == lax.broadcasted_iota(jnp.int32, (LANES, depth), 0)).astype(F32).astype(BF)

    def project_temporal(blocks):
        for i, (j, f, chunk) in enumerate(blocks):
            value = mid[0, f, chunk] if j == 0 else mids[j - 1, f, chunk]
            nb[i * blk:(i + 1) * blk] = normalize(value, gain_two)
        count = len(blocks) * blk
        per = depth // TILE

        def step(i, carry):
            at = pl.ds(pl.multiple_of(i * TILE, TILE), TILE)
            lanes = pl.ds(pl.multiple_of(i % per * TILE, TILE), TILE)
            got = jnp.dot(nb[:count], w2[:, at], preferred_element_type=F32).astype(BF)
            for k, (j, f, chunk) in enumerate(blocks):
                qkv[i // per, chunk, j * frames + f, :, lanes] = got[k * blk:(k + 1) * blk]
            return carry

        lax.fori_loop(0, 3 * per, step, 0, unroll=True)

    ready("w2", "order", "gain2")
    project_temporal([(0, f, chunk) for f in range(frames) for chunk in range(chunks)])
    final = frames - 1
    for f in range(final):
        for j in away:
            for chunk in range(chunks):
                m_copies[f, chunk, j].wait_recv()
        project_temporal([(j, f, chunk) for j in away for chunk in range(chunks)])

    def frame_rank(slot):
        return order_ref[(t - slot // frames) % ranks * frames + slot % frames]

    k_order = [frame_rank(g) for g in range(keys)]

    def attend_temporal(chunk):
        def step(f, carry):
            q = qkv[0, chunk, f] * BF(SCALE)
            products = jnp.concatenate([q * qkv[1, chunk, g] for g in range(keys)], axis=0)
            scores = jnp.dot(products, gather[...], preferred_element_type=F32)
            own_order = frame_rank(f)
            kept = [scores[g * blk:(g + 1) * blk] + jnp.where(k_order[g] <= own_order, 0.0, -1e30)
                    for g in range(keys)]
            top_score = functools.reduce(jnp.maximum, kept)
            exps = [jnp.exp(sc - top_score) for sc in kept]
            scale = 1.0 / functools.reduce(jnp.add, exps)
            weights = jnp.concatenate([(e * scale).astype(BF) for e in exps], axis=0)
            spreads = jnp.dot(weights, spread[...], preferred_element_type=F32)
            total = None
            for g in range(keys):
                term = spreads[g * blk:(g + 1) * blk] * qkv[2, chunk, g].astype(F32)
                total = term if total is None else total + term
            ctx2[0, chunk, f] = total.astype(BF)
            return carry

        lax.fori_loop(0, keys, step, 0, unroll=4)

    row_tile = 1024
    sub = depth // (ranks * places * ny)
    stacked = keys * blk

    def add_gradient(terms, first, final):
        def step(i, carry):
            at = pl.ds(pl.multiple_of(i * row_tile, row_tile), row_tile)
            left = jnp.concatenate([ctx2[w, c, :, :, at].reshape(stacked, row_tile) for w, c in terms], axis=0)
            right = jnp.concatenate([cot[w, c].reshape(stacked, half) for w, c in terms], axis=0)
            got = lax.dot_general(left, right, (((0,), (0,)), ((), ())), preferred_element_type=F32)
            if not first:
                got = got + accf[at]
            if final:
                acc[at] = got.astype(BF)
            else:
                accf[at] = got
            return carry

        lax.fori_loop(0, depth // row_tile, step, 0)

    def merge_temporal(chunk):
        got = jnp.dot(ctx2[0, chunk].reshape(stacked, depth), o2[...], preferred_element_type=F32)
        for j in range(ranks):
            for f in range(frames):
                base = (j * frames + f) * blk
                value = mid[0, f, chunk] if j == 0 else mids[j - 1, f, chunk]
                value = (value.astype(F32) + got[base:base + blk]).astype(BF).reshape(inner + (depth,))
                if j == 0:
                    out[f, chunk, :, t] = value
                else:
                    sent[j - 1, chunk, f] = value

    out_copies = []
    returns = {chunk: [(chunk, f, j) for f in range(frames) for j in away] for chunk in order}

    def return_output(some):
        for chunk, f, j in some:
            copy = remote(sent.at[j - 1, chunk, f], out.at[f, chunk, :, t], s_os.at[chunk, f, j - 1],
                          s_or.at[chunk, f, j - 1], "tm", (t - j) % ranks)
            copy.start()
            out_copies.append(copy)

    c_copies = {}
    ready(*[f"cot{f}" for f in range(frames)])
    ready("o2")
    before = None
    for chunk in order:
        for j in away:
            m_copies[final, chunk, j].wait_recv()
        project_temporal([(j, final, chunk) for j in away])
        attend_temporal(chunk)
        c_copies[chunk] = remote(ctx2.at[0, chunk], ctx2.at[1, chunk], s_cs.at[chunk], s_cr.at[chunk],
                                 "batch", other_core)
        c_copies[chunk].start()
        for of, copy in cot_copies:
            if of == chunk:
                copy.wait_recv()
        if before is not None:
            c_copies[before].wait_recv()
        add_gradient([(0, chunk)] + ([(1, before)] if before is not None else []), before is None, False)
        if chunk != order[-1]:
            merge_temporal(chunk)
            return_output(returns[chunk][:len(returns[chunk]) // 2])
        before = chunk
    c_copies[before].wait_recv()
    add_gradient([(1, before)], chunks == 0, True)

    sems = iter(range(s_gs.shape[0]))
    axes = {"x": ("tm", t, ranks, lambda to: to), "z": ("space", s, places, lambda to: to),
            "y": ("batch", y, ny, lambda to: to * 2 + core)}
    column = lambda n: slice(n * LANES, (n + 1) * LANES)
    count = half // LANES
    grid = acc.reshape(ranks, places, ny, sub, half)

    def exchange(axis, source, dests):
        name, me, size, device = axes[axis]
        copies = []
        for k in range(1, size):
            to = (me + k) % size
            n = next(sems)
            copy = remote(source(to), dests.at[k - 1], s_gs.at[n], s_gr.at[n], name, device(to))
            copy.start()
            copies.append(copy)
        return copies

    def place_in(n, stage, value):
        route = ROUTES[n]
        left = [a for a in "xzy" if a not in route[:stage]]
        at = tuple(value if a == route[stage] else slice(None) for a in left)
        return at + (slice(None), column(n)) if stage == 0 else at

    flying = {}

    def launch(n, stage):
        src = grid if stage == 0 else summed[3 * n + stage - 1]
        flying[n, stage] = exchange(ROUTES[n][stage], lambda to: src.at[place_in(n, stage, to)],
                                    arrived[3 * n + stage])

    def finish(n, stage):
        for copy in flying[n, stage]:
            copy.wait()
        src = grid if stage == 0 else summed[3 * n + stage - 1]
        _, me, size, _ = axes[ROUTES[n][stage]]
        total = src[place_in(n, stage, me)].astype(F32)
        for k in range(size - 1):
            total = total + arrived[3 * n + stage][k].astype(F32)
        summed[3 * n + stage][...] = total.astype(BF)
        if stage < 2:
            launch(n, stage + 1)

    def place_piece(n, owner, value):
        rows_at = pl.ds(pl.multiple_of(owner // 2 * sub, sub), sub)
        lanes = pl.ds(pl.multiple_of(owner % 2 * half + n * LANES, LANES), LANES)
        grad[rows_at, lanes] = value.astype(F32)

    last = {}

    def gather_piece(n):
        piece = summed[3 * n + 2]
        last[n] = []
        for k in range(1, parts):
            at = next(sems)
            copy = remote(piece, gr.at[n, k - 1], s_gs.at[at], s_gr.at[at], "batch", (b + k) % parts)
            copy.start()
            last[n].append(copy)
        place_piece(n, b, piece[...])

    for n in range(count):
        launch(n, 0)

    for chunk in order[:-1]:
        return_output(returns[chunk][len(returns[chunk]) // 2:])
    merge_temporal(order[-1])
    for n, stage in WAITS:
        finish(n, stage)
        if (n, stage) == (2, 0):
            return_output(returns[order[-1]])
        if stage == 2:
            gather_piece(n)
    for n in last:
        for k, copy in enumerate(last[n]):
            copy.wait()
            place_piece(n, (b - 1 - k) % parts, gr[n, k])

    for copy in out_copies:
        copy.wait_recv()
    for copies in (x_copies, m_copies, c_copies):
        for copy in copies.values():
            copy.wait_send()
    for _, copy in cot_copies:
        copy.wait_send()
    for copy in out_copies:
        copy.wait_send()
    for f in range(frames):
        for j in range(ranks):
            finish_halo(f, j)


def write_kernel(out_v, grad_v, out, grad, sems):
    copies = [pltpu.make_async_copy(out_v, out, sems.at[0]), pltpu.make_async_copy(grad_v, grad, sems.at[1])]
    for copy in copies:
        copy.start()
    for copy in copies:
        copy.wait()


def per_device(clip_tokens, frame_order, row_reach, spatial_gain, spatial_heads, spatial_merge,
               temporal_gain, temporal_heads, temporal_merge, cotangent):
    ranks, places, parts = lax.axis_size("tm"), lax.axis_size("space"), lax.axis_size("batch")
    _, all_frames, rows, pc, depth = clip_tokens.shape
    frames, cols = all_frames // ranks, pc * ranks
    chunks, blk = rows // HALO, HALO * pc
    span = blk * ranks
    keys = ranks * frames
    ny = parts // 2
    half = depth // 2
    sub = depth // (ranks * places * ny)
    chunks_of = half // LANES
    inner = (HALO, pc) if pc % 16 == 0 else (1, blk)
    dims = (ranks, places, parts, frames, chunks, pc, depth, inner)
    anywhere = pl.BlockSpec(memory_space=pl.ANY)
    vmem = pl.BlockSpec(memory_space=pltpu.VMEM)
    dma = pltpu.SemaphoreType.DMA
    others = max(ranks - 1, 1)
    most = max(frames * chunks * blk, 2 * ranks * blk, (ranks - 1) * max(chunks, 2) * blk,
               (ranks - 1) * chunks * blk)
    sizes = {"x": ranks, "z": places, "y": ny}
    arrivals, sums, steps = [], [], 0
    for route in ROUTES:
        for stage in range(3):
            left = tuple(sizes[a] for a in "xzy" if a not in route[:stage + 1])
            arrivals.append(pltpu.VMEM((max(sizes[route[stage]] - 1, 1),) + left + (sub, LANES), BF))
            sums.append(pltpu.VMEM(left + (sub, LANES), BF))
            steps += sizes[route[stage]] - 1
        steps += parts - 1
    scratch = [
        pltpu.VMEM((frames, chunks + 2, ranks, blk, depth), BF),
        pltpu.VMEM((others, frames, chunks, blk, depth), BF),
        pltpu.VMEM((3, frames, chunks + 2, ranks, blk, depth), BF),
        pltpu.VMEM((most, depth), BF),
        pltpu.VMEM((depth, 3 * depth), BF),
        pltpu.VMEM((depth, depth), BF),
        pltpu.VMEM((depth, 3 * depth), BF),
        pltpu.VMEM((depth, depth), BF),
        pltpu.VMEM((span, depth), BF),
        pltpu.VMEM((ranks, frames, chunks, blk, depth), BF),
        pltpu.VMEM((others, frames, chunks, blk, depth), BF),
        pltpu.VMEM((3, chunks, keys, blk, depth), BF),
        pltpu.VMEM((2, chunks, keys, blk, depth), BF),
        pltpu.VMEM((2, chunks, keys) + inner + (half,), BF),
        pltpu.VMEM((depth, LANES), BF),
        pltpu.VMEM((LANES, depth), BF),
        pltpu.VMEM((frames, chunks, span, 3 * span), F32),
        pltpu.VMEM((depth, half), F32),
        pltpu.VMEM((depth, half), BF),
        pltpu.VMEM((chunks_of, parts - 1, sub, LANES), BF),
        pltpu.VMEM((others, chunks, frames) + inner + (depth,), BF),
        pltpu.SMEM((all_frames,), jnp.int32),
        pltpu.SMEM((frames,), jnp.int32),
        pltpu.VMEM((1, depth), F32),
        pltpu.VMEM((1, depth), F32),
        *arrivals, *sums,
        dma((2 * frames + 10 + (ranks - 1) * frames,)),
        dma((frames, chunks, others)), dma((frames, chunks, others)),
        dma((2, frames, ranks)), dma((2, frames, ranks)),
        dma((frames, chunks, others)), dma((frames, chunks, others)),
        dma((2, chunks, ranks)), dma((2, chunks, ranks)),
        dma((chunks,)), dma((chunks,)),
        dma((chunks, frames, others)), dma((chunks, frames, others)),
        dma((steps,)), dma((steps,)),
    ]
    by_columns = cotangent.reshape(frames, chunks, HALO, ranks, pc, depth)
    if inner[0] == 1:
        by_columns = by_columns.transpose(0, 1, 3, 2, 4, 5).reshape(frames, chunks, 1, ranks, blk, depth)
    out, grad = pl.pallas_call(
        functools.partial(block_kernel, dims),
        out_shape=(pltpu.VMEM((frames, chunks, inner[0], ranks, inner[1], depth), BF),
                   pltpu.VMEM((ny * sub, depth), F32)),
        in_specs=[anywhere] * 10,
        out_specs=(vmem, vmem),
        scratch_shapes=scratch,
        compiler_params=pltpu.CompilerParams(collective_id=0, has_side_effects=True,
                                             vmem_limit_bytes=60 << 20),
        name="block",
    )(clip_tokens.reshape(all_frames, chunks, blk, depth), frame_order.reshape(-1), row_reach.reshape(-1),
      spatial_gain.reshape(1, depth), temporal_gain.reshape(1, depth),
      spatial_heads, spatial_merge, temporal_heads, temporal_merge, by_columns)
    out, grad = pl.pallas_call(
        write_kernel,
        out_shape=(jax.ShapeDtypeStruct(out.shape, BF), jax.ShapeDtypeStruct(grad.shape, F32)),
        in_specs=[vmem, vmem],
        out_specs=(anywhere, anywhere),
        scratch_shapes=[dma((2,))],
        name="write",
    )(pltpu.with_memory_space_constraint(out, pltpu.VMEM), pltpu.with_memory_space_constraint(grad, pltpu.VMEM))
    if inner[0] == 1:
        out = out.reshape(frames, chunks, ranks, HALO, pc, depth).transpose(0, 1, 3, 2, 4, 5)
    return out.reshape(1, frames, rows, cols, depth), grad


def solution(mesh):
    in_specs = (
        P("batch", None, "space", "tm", None),
        P("batch", None),
        P("batch", "tm"),
        P(),
        P(),
        P(),
        P(),
        P(),
        P(),
        P("batch", "tm", "space", None, None),
    )
    out_specs = (P("batch", "tm", "space", None, None), P(("tm", "space"), None))
    return jax.shard_map(per_device, mesh=mesh, in_specs=in_specs, out_specs=out_specs, check_vma=False)
```

```python
import functools

import jax
import jax.numpy as jnp
from jax import lax
from jax.experimental import pallas as pl
from jax.experimental.pallas import tpu as pltpu
from jax.sharding import PartitionSpec as P

HALO = 4
HEADS = 16
HEAD_DIM = 64
LANES = 128
TILE = 1024
UNROLL = 8
ROUTES = ("xyz", "yxz", "zxy", "yxz")
WAITS = ((0, 0), (1, 0), (3, 0), (1, 1), (0, 1), (2, 0), (3, 1), (2, 1), (0, 2), (1, 2), (2, 2), (3, 2))
SCALE = HEAD_DIM ** (-0.5)
FLOOR = 0.5
BF = jnp.bfloat16
F32 = jnp.float32
MESH = pl.DeviceIdType.MESH


def block_kernel(dims, *refs):
    ranks, places, parts, frames, chunks, pc, depth, inner = dims
    every = (slice(None), slice(None))
    (clip, order_in, reach_in, gain_one_in, gain_two_in, w_one, m_one, w_two, m_two, cot_in,
     out, grad,
     xx, away_x, pr, nb, w1, o1, w2, o2, ctx1, mid, mids, qkv, ctx2, cot, gather, spread, bias, accf, acc,
     gr, sent, order_ref, reach_ref, gain_one, gain_two, *rest) = refs
    arrived, summed = rest[:3 * len(ROUTES)], rest[3 * len(ROUTES):6 * len(ROUTES)]
    (s_load, s_xs, s_xr, s_zs, s_zr, s_ms, s_mr, s_ts, s_tr, s_cs, s_cr, s_os, s_or, s_gs, s_gr) = rest[6 * len(ROUTES):]
    blk = HALO * pc
    span = blk * ranks
    rows = chunks * HALO
    keys = ranks * frames
    half = depth // 2
    t, s, b = lax.axis_index("tm"), lax.axis_index("space"), lax.axis_index("batch")
    core, y = b % 2, b // 2
    ny = parts // 2

    loads = {}

    def load(name, src, dst):
        copy = pltpu.make_async_copy(src, dst, s_load.at[len(loads)])
        copy.start()
        loads[name] = copy

    def ready(*names):
        for name in names:
            loads[name].wait()

    def half_of(which):
        return pl.ds(pl.multiple_of(which * half, half), half)

    for f in range(frames):
        load(f"x{f}", clip.at[t * frames + f], xx.at[f, 1:chunks + 1, t])
        for j in range(1, ranks):
            load(f"y{f}{j}", clip.at[(t + j) % ranks * frames + f], away_x.at[j - 1, f])
    for name, src, dst in (("reach", reach_in, reach_ref), ("order", order_in, order_ref),
                           ("gain1", gain_one_in, gain_one), ("gain2", gain_two_in, gain_two)):
        load(name, src, dst)
    for part in range(3):
        load(f"w1{part}", w_one.at[:, part * depth:(part + 1) * depth], w1.at[:, part * depth:(part + 1) * depth])
    load("o1", m_one, o1)
    load("w2", w_two, w2)
    load("o2", m_two, o2)
    for f in range(frames):
        load(f"cot{f}", cot_in.at[f, :, :, t, :, half_of(core)], cot.at[0, :, f])

    barrier = pltpu.get_barrier_semaphore()
    for axis, me, count in (("tm", t, ranks), ("space", s, places), ("batch", b, parts)):
        for shift in range(1, count):
            pl.semaphore_signal(barrier, inc=1, device_id={axis: (me + shift) % count}, device_id_type=MESH)
    other_core = b + 1 - 2 * core
    for j in range(1, ranks):
        pl.semaphore_signal(barrier, inc=1, device_id={"tm": (t + j) % ranks, "batch": other_core},
                            device_id_type=MESH)
    pl.semaphore_wait(barrier, 2 * ranks + places + parts - 4)

    ready(*[f"x{f}" for f in range(frames)], *[f"y{f}{j}" for f in range(frames) for j in range(1, ranks)])
    def remote(src, dst, send, recv, axis, to):
        return pltpu.make_async_remote_copy(src, dst, send, recv, device_id={axis: to}, device_id_type=MESH)

    x_copies = {}
    for f in range(frames):
        for chunk in range(chunks):
            for j in range(1, ranks):
                to = (t + j) % ranks
                copy = remote(away_x.at[j - 1, f, chunk], xx.at[f, 1 + chunk, t],
                              s_xs.at[f, chunk, j - 1], s_xr.at[f, chunk, j - 1], "tm", to)
                copy.start()
                x_copies[f, chunk, j] = copy

    def halo(f, j, up):
        source = (t - j) % ranks
        slot, dest = (1, chunks + 1) if up else (chunks, 0)
        return remote(xx.at[f, slot, source], xx.at[f, dest, source], s_zs.at[int(up), f, j], s_zr.at[int(up), f, j],
                      "space", (s - 1) if up else (s + 1))

    def send_halo(f, j, up):
        @pl.when((s > 0) if up else (s < places - 1))
        def _():
            halo(f, j, up).start()

    def wait_halo(f, j, sides=(False, True)):
        for up in sides:
            @pl.when((s < places - 1) if up else (s > 0))
            def _():
                halo(f, j, up).wait_recv()

    def finish_halo(f, j):
        @pl.when(s > 0)
        def _():
            halo(f, j, True).wait_send()

        @pl.when(s < places - 1)
        def _():
            halo(f, j, False).wait_send()

    def forward(f, chunk):
        for j in range(1, ranks):
            x_copies[f, chunk, j].wait_recv()
            if chunk == 0:
                send_halo(f, j, True)
            if chunk == chunks - 1:
                send_halo(f, j, False)
        if f + 1 < frames and chunk == 0:
            send_halo(f + 1, 0, True)
        if f + 1 < frames and chunk == chunks - 1:
            send_halo(f + 1, 0, False)

    send_halo(0, 0, True)
    send_halo(0, 0, False)
    cot_copies = []

    def send_cotangent(chunk, shifts):
        for j in shifts:
            to = (t + j) % ranks
            for which, core_to in ((0, core), (1, 1 - core)):
                if j == 0 and which == 0:
                    continue
                copy = pltpu.make_async_remote_copy(
                    cot_in.at[:, chunk, :, to, :, half_of(core_to)],
                    cot.at[which, chunk, j * frames:(j + 1) * frames],
                    s_ts.at[which, chunk, j], s_tr.at[which, chunk, j],
                    device_id={"tm": to, "batch": b - core + core_to}, device_id_type=MESH)
                copy.start()
                cot_copies.append((chunk, copy))

    order = list(reversed(range(chunks)))
    for chunk in order:
        send_cotangent(chunk, range(1))
    for chunk in order[:-1]:
        send_cotangent(chunk, range(1, ranks))

    @pl.when(s == 0)
    def _():
        xx[:, 0] = jnp.zeros((frames, ranks, blk, depth), BF)

    @pl.when(s == places - 1)
    def _():
        xx[:, chunks + 1] = jnp.zeros((frames, ranks, blk, depth), BF)

    ready("reach", "gain1")
    lane = lax.broadcasted_iota(jnp.int32, (1, LANES), 1)
    first_head = (lane < HEAD_DIM).astype(F32)
    masks = (first_head.astype(BF), (1.0 - first_head).astype(BF))
    for f in range(frames):
        for chunk in range(chunks):
            shape = (span, 3 * span)
            q_row = chunk * HALO + lax.broadcasted_iota(jnp.int32, shape, 0) % blk // pc
            k_at = lax.broadcasted_iota(jnp.int32, shape, 1)
            k_row = (chunk - 1 + k_at // span) * HALO + k_at % blk // pc
            place = s * rows + k_row
            kept = (jnp.abs(k_row - q_row) <= reach_ref[f]) & (place >= 0) & (place < rows * places)
            bias[f, chunk] = jnp.where(kept, 0.0, -1e30)

    def normalize(values, gain):
        widened = values.astype(F32)
        scaled = widened * lax.rsqrt(jnp.mean(widened * widened, axis=-1, keepdims=True) + FLOOR)
        return (scaled * gain[...]).astype(BF)

    def project_spatial(blocks, first):
        for i, (f, slot, source) in enumerate(blocks):
            nb[i * blk:(i + 1) * blk] = normalize(xx[f, slot, source], gain_one)
        count = len(blocks) * blk
        per = depth // TILE

        def step(i, carry):
            at = pl.ds(pl.multiple_of(i * TILE, TILE), TILE)
            lanes = pl.ds(pl.multiple_of(i % per * TILE, TILE), TILE)
            got = jnp.dot(nb[:count], w1[:, at], preferred_element_type=F32).astype(BF)
            for k, (f, slot, source) in enumerate(blocks):
                pr[i // per, f, slot, source, :, lanes] = got[k * blk:(k + 1) * blk]
            return carry

        lax.fori_loop(first * per, 3 * per, step, 0, unroll=True)

    own = range(1, chunks + 1)
    ends = (0, chunks + 1)
    away = range(1, ranks)

    def attend_spatial(f, chunk):
        ones = jnp.ones((3 * span, LANES), BF)

        def pair_step(i, carry):
            for u in range(UNROLL):
                at = pl.ds(pl.multiple_of((UNROLL * i + u) * LANES, LANES), LANES)
                q = pr[0, f, 1 + chunk, :, :, at].reshape(span, LANES) * BF(SCALE)
                both = jnp.concatenate([q * masks[0], q * masks[1]], axis=0)
                k = pr[1, f, chunk:chunk + 3, :, :, at].reshape(3 * span, LANES)
                v = pr[2, f, chunk:chunk + 3, :, :, at].reshape(3 * span, LANES)
                sc = lax.dot_general(both, k, (((1,), (1,)), ((), ())), preferred_element_type=F32)
                sc = sc + jnp.concatenate([bias[f, chunk], bias[f, chunk]], axis=0)
                p = jnp.exp(sc - jnp.max(sc, axis=-1, keepdims=True)).astype(BF)
                o = jnp.dot(p, jnp.concatenate([v, ones], axis=1), preferred_element_type=F32)
                o = jnp.where(jnp.concatenate([lane, lane], axis=1) % LANES < HEAD_DIM, o[:span], o[span:])
                ctx1[:, at] = (o[:, :LANES] / o[:, LANES:]).astype(BF)
            return carry

        lax.fori_loop(0, depth // LANES // UNROLL, pair_step, 0)

    m_copies = {}

    def merge_spatial(f, chunk):
        def step(i, carry):
            at = pl.ds(pl.multiple_of(i * TILE, TILE), TILE)
            got = jnp.dot(ctx1[...], o1[:, at], preferred_element_type=F32)
            for source in range(ranks):
                base = source * blk
                total = got[base:base + blk] + xx[f, 1 + chunk, source, :, at].astype(F32)
                mid[(source - t) % ranks, f, chunk, :, at] = total.astype(BF)
            return carry

        lax.fori_loop(0, depth // TILE, step, 0)
        for j in away:
            copy = remote(mid.at[j, f, chunk], mids.at[j - 1, f, chunk], s_ms.at[f, chunk, j - 1],
                          s_mr.at[f, chunk, j - 1], "tm", (t + j) % ranks)
            copy.start()
            m_copies[f, chunk, j] = copy

    ready("w10", "w11", "w12")
    project_spatial([(f, slot, t) for f in range(frames) for slot in own], 0)
    for chunk in range(chunks - 1):
        forward(0, chunk)
    wait_halo(0, 0)
    project_spatial([(0, slot, t) for slot in ends], 1)
    forward(0, chunks - 1)
    project_spatial([(0, slot, (t - j) % ranks) for j in away for slot in own], 0)
    ready("o1")
    for f in range(frames):
        if f == 0:
            for j in away:
                wait_halo(f, j, (True,))
            project_spatial([(f, chunks + 1, (t - j) % ranks) for j in away], 1)
        else:
            for j in range(ranks):
                wait_halo(f, j)
            project_spatial([(f, slot, (t - j) % ranks) for j in range(ranks) for slot in ends], 1)
        for chunk in reversed(range(chunks)):
            if f == 0 and chunk == 0:
                for j in away:
                    wait_halo(f, j, (False,))
                project_spatial([(f, 0, (t - j) % ranks) for j in away], 1)
            if f + 1 < frames and chunk == 0:
                forward(f + 1, chunks - 1)
            attend_spatial(f, chunk)
            if f + 1 < frames and chunk == chunks - 1:
                for early in range(chunks - 1):
                    forward(f + 1, early)
            merge_spatial(f, chunk)
        if f + 1 < frames:
            project_spatial([(f + 1, slot, (t - j) % ranks) for j in away for slot in own], 0)

    for chunk in order[-1:]:
        send_cotangent(chunk, range(1, ranks))
    head = lax.broadcasted_iota(jnp.int32, (depth, LANES), 0) // HEAD_DIM
    gather[...] = (head == lax.broadcasted_iota(jnp.int32, (depth, LANES), 1)).astype(F32).astype(BF)
    head = lax.broadcasted_iota(jnp.int32, (LANES, depth), 1) // HEAD_DIM
    spread[...] = (head == lax.broadcasted_iota(jnp.int32, (LANES, depth), 0)).astype(F32).astype(BF)

    def project_temporal(blocks):
        for i, (j, f, chunk) in enumerate(blocks):
            value = mid[0, f, chunk] if j == 0 else mids[j - 1, f, chunk]
            nb[i * blk:(i + 1) * blk] = normalize(value, gain_two)
        count = len(blocks) * blk
        per = depth // TILE

        def step(i, carry):
            at = pl.ds(pl.multiple_of(i * TILE, TILE), TILE)
            lanes = pl.ds(pl.multiple_of(i % per * TILE, TILE), TILE)
            got = jnp.dot(nb[:count], w2[:, at], preferred_element_type=F32).astype(BF)
            for k, (j, f, chunk) in enumerate(blocks):
                qkv[i // per, chunk, j * frames + f, :, lanes] = got[k * blk:(k + 1) * blk]
            return carry

        lax.fori_loop(0, 3 * per, step, 0, unroll=True)

    ready("w2", "order", "gain2")
    project_temporal([(0, f, chunk) for f in range(frames) for chunk in range(chunks)])
    final = frames - 1
    for f in range(final):
        for j in away:
            for chunk in range(chunks):
                m_copies[f, chunk, j].wait_recv()
        project_temporal([(j, f, chunk) for j in away for chunk in range(chunks)])

    def frame_rank(slot):
        return order_ref[(t - slot // frames) % ranks * frames + slot % frames]

    k_order = [frame_rank(g) for g in range(keys)]

    def attend_temporal(chunk):
        def step(f, carry):
            q = qkv[0, chunk, f] * BF(SCALE)
            products = jnp.concatenate([q * qkv[1, chunk, g] for g in range(keys)], axis=0)
            scores = jnp.dot(products, gather[...], preferred_element_type=F32)
            own_order = frame_rank(f)
            kept = [scores[g * blk:(g + 1) * blk] + jnp.where(k_order[g] <= own_order, 0.0, -1e30)
                    for g in range(keys)]
            top_score = functools.reduce(jnp.maximum, kept)
            exps = [jnp.exp(sc - top_score) for sc in kept]
            scale = 1.0 / functools.reduce(jnp.add, exps)
            weights = jnp.concatenate([(e * scale).astype(BF) for e in exps], axis=0)
            spreads = jnp.dot(weights, spread[...], preferred_element_type=F32)
            total = None
            for g in range(keys):
                term = spreads[g * blk:(g + 1) * blk] * qkv[2, chunk, g].astype(F32)
                total = term if total is None else total + term
            ctx2[0, chunk, f] = total.astype(BF)
            return carry

        lax.fori_loop(0, keys, step, 0, unroll=4)

    row_tile = 1024
    sub = depth // (ranks * places * ny)
    stacked = keys * blk

    def add_gradient(terms, first, final):
        def step(i, carry):
            at = pl.ds(pl.multiple_of(i * row_tile, row_tile), row_tile)
            left = jnp.concatenate([ctx2[w, c, :, :, at].reshape(stacked, row_tile) for w, c in terms], axis=0)
            right = jnp.concatenate([cot[w, c].reshape(stacked, half) for w, c in terms], axis=0)
            got = lax.dot_general(left, right, (((0,), (0,)), ((), ())), preferred_element_type=F32)
            if not first:
                got = got + accf[at]
            if final:
                acc[at] = got.astype(BF)
            else:
                accf[at] = got
            return carry

        lax.fori_loop(0, depth // row_tile, step, 0)

    def merge_temporal(chunk):
        got = jnp.dot(ctx2[0, chunk].reshape(stacked, depth), o2[...], preferred_element_type=F32)
        for j in range(ranks):
            for f in range(frames):
                base = (j * frames + f) * blk
                value = mid[0, f, chunk] if j == 0 else mids[j - 1, f, chunk]
                value = (value.astype(F32) + got[base:base + blk]).astype(BF).reshape(inner + (depth,))
                if j == 0:
                    out[f, chunk, :, t] = value
                else:
                    sent[j - 1, chunk, f] = value

    out_copies = []
    returns = {chunk: [(chunk, f, j) for f in range(frames) for j in away] for chunk in order}

    def return_output(some):
        for chunk, f, j in some:
            copy = remote(sent.at[j - 1, chunk, f], out.at[f, chunk, :, t], s_os.at[chunk, f, j - 1],
                          s_or.at[chunk, f, j - 1], "tm", (t - j) % ranks)
            copy.start()
            out_copies.append(copy)

    c_copies = {}
    ready(*[f"cot{f}" for f in range(frames)])
    ready("o2")
    before = None
    for chunk in order:
        for j in away:
            m_copies[final, chunk, j].wait_recv()
        project_temporal([(j, final, chunk) for j in away])
        attend_temporal(chunk)
        c_copies[chunk] = remote(ctx2.at[0, chunk], ctx2.at[1, chunk], s_cs.at[chunk], s_cr.at[chunk],
                                 "batch", other_core)
        c_copies[chunk].start()
        for of, copy in cot_copies:
            if of == chunk:
                copy.wait_recv()
        if before is not None:
            c_copies[before].wait_recv()
        add_gradient([(0, chunk)] + ([(1, before)] if before is not None else []), before is None, False)
        if chunk != order[-1]:
            merge_temporal(chunk)
            return_output(returns[chunk][:len(returns[chunk]) // 2])
        before = chunk
    c_copies[before].wait_recv()
    add_gradient([(1, before)], chunks == 0, True)

    sems = iter(range(s_gs.shape[0]))
    axes = {"x": ("tm", t, ranks, lambda to: to), "z": ("space", s, places, lambda to: to),
            "y": ("batch", y, ny, lambda to: to * 2 + core)}
    column = lambda n: slice(n * LANES, (n + 1) * LANES)
    count = half // LANES
    grid = acc.reshape(ranks, places, ny, sub, half)

    def exchange(axis, source, dests):
        name, me, size, device = axes[axis]
        copies = []
        for k in range(1, size):
            to = (me + k) % size
            n = next(sems)
            copy = remote(source(to), dests.at[k - 1], s_gs.at[n], s_gr.at[n], name, device(to))
            copy.start()
            copies.append(copy)
        return copies

    def place_in(n, stage, value):
        route = ROUTES[n]
        left = [a for a in "xzy" if a not in route[:stage]]
        at = tuple(value if a == route[stage] else slice(None) for a in left)
        return at + (slice(None), column(n)) if stage == 0 else at

    flying = {}

    def launch(n, stage):
        src = grid if stage == 0 else summed[3 * n + stage - 1]
        flying[n, stage] = exchange(ROUTES[n][stage], lambda to: src.at[place_in(n, stage, to)],
                                    arrived[3 * n + stage])

    def finish(n, stage):
        for copy in flying[n, stage]:
            copy.wait()
        src = grid if stage == 0 else summed[3 * n + stage - 1]
        _, me, size, _ = axes[ROUTES[n][stage]]
        total = src[place_in(n, stage, me)].astype(F32)
        for k in range(size - 1):
            total = total + arrived[3 * n + stage][k].astype(F32)
        summed[3 * n + stage][...] = total.astype(BF)
        if stage < 2:
            launch(n, stage + 1)

    def place_piece(n, owner, value):
        rows_at = pl.ds(pl.multiple_of(owner // 2 * sub, sub), sub)
        lanes = pl.ds(pl.multiple_of(owner % 2 * half + n * LANES, LANES), LANES)
        grad[rows_at, lanes] = value.astype(F32)

    last = {}

    def gather_piece(n):
        piece = summed[3 * n + 2]
        last[n] = []
        for k in range(1, parts):
            at = next(sems)
            copy = remote(piece, gr.at[n, k - 1], s_gs.at[at], s_gr.at[at], "batch", (b + k) % parts)
            copy.start()
            last[n].append(copy)
        place_piece(n, b, piece[...])

    for n in range(count):
        launch(n, 0)

    for chunk in order[:-1]:
        return_output(returns[chunk][len(returns[chunk]) // 2:])
    merge_temporal(order[-1])
    for n, stage in WAITS:
        finish(n, stage)
        if (n, stage) == (2, 0):
            return_output(returns[order[-1]])
        if stage == 2:
            gather_piece(n)
    for n in last:
        for k, copy in enumerate(last[n]):
            copy.wait()
            place_piece(n, (b - 1 - k) % parts, gr[n, k])

    for copy in out_copies:
        copy.wait_recv()
    for copies in (x_copies, m_copies, c_copies):
        for copy in copies.values():
            copy.wait_send()
    for _, copy in cot_copies:
        copy.wait_send()
    for copy in out_copies:
        copy.wait_send()
    for f in range(frames):
        for j in range(ranks):
            finish_halo(f, j)


def write_kernel(out_v, grad_v, out, grad, sems):
    frames, chunks = out_v.shape[:2]
    copies = [pltpu.make_async_copy(grad_v, grad, sems.at[frames * chunks])]
    for f in range(frames):
        for chunk in range(chunks):
            copies.append(pltpu.make_async_copy(out_v.at[f, chunk], out.at[f, chunk], sems.at[f * chunks + chunk]))
    for copy in copies:
        copy.start()
    for copy in copies:
        copy.wait()


def per_device(clip_tokens, frame_order, row_reach, spatial_gain, spatial_heads, spatial_merge,
               temporal_gain, temporal_heads, temporal_merge, cotangent):
    ranks, places, parts = lax.axis_size("tm"), lax.axis_size("space"), lax.axis_size("batch")
    _, all_frames, rows, pc, depth = clip_tokens.shape
    frames, cols = all_frames // ranks, pc * ranks
    chunks, blk = rows // HALO, HALO * pc
    span = blk * ranks
    keys = ranks * frames
    ny = parts // 2
    half = depth // 2
    sub = depth // (ranks * places * ny)
    chunks_of = half // LANES
    inner = (HALO, pc) if pc % 16 == 0 else (1, blk)
    dims = (ranks, places, parts, frames, chunks, pc, depth, inner)
    anywhere = pl.BlockSpec(memory_space=pl.ANY)
    vmem = pl.BlockSpec(memory_space=pltpu.VMEM)
    dma = pltpu.SemaphoreType.DMA
    others = max(ranks - 1, 1)
    most = max(frames * chunks * blk, 2 * ranks * blk, (ranks - 1) * max(chunks, 2) * blk,
               (ranks - 1) * chunks * blk)
    sizes = {"x": ranks, "z": places, "y": ny}
    arrivals, sums, steps = [], [], 0
    for route in ROUTES:
        for stage in range(3):
            left = tuple(sizes[a] for a in "xzy" if a not in route[:stage + 1])
            arrivals.append(pltpu.VMEM((max(sizes[route[stage]] - 1, 1),) + left + (sub, LANES), BF))
            sums.append(pltpu.VMEM(left + (sub, LANES), BF))
            steps += sizes[route[stage]] - 1
        steps += parts - 1
    scratch = [
        pltpu.VMEM((frames, chunks + 2, ranks, blk, depth), BF),
        pltpu.VMEM((others, frames, chunks, blk, depth), BF),
        pltpu.VMEM((3, frames, chunks + 2, ranks, blk, depth), BF),
        pltpu.VMEM((most, depth), BF),
        pltpu.VMEM((depth, 3 * depth), BF),
        pltpu.VMEM((depth, depth), BF),
        pltpu.VMEM((depth, 3 * depth), BF),
        pltpu.VMEM((depth, depth), BF),
        pltpu.VMEM((span, depth), BF),
        pltpu.VMEM((ranks, frames, chunks, blk, depth), BF),
        pltpu.VMEM((others, frames, chunks, blk, depth), BF),
        pltpu.VMEM((3, chunks, keys, blk, depth), BF),
        pltpu.VMEM((2, chunks, keys, blk, depth), BF),
        pltpu.VMEM((2, chunks, keys) + inner + (half,), BF),
        pltpu.VMEM((depth, LANES), BF),
        pltpu.VMEM((LANES, depth), BF),
        pltpu.VMEM((frames, chunks, span, 3 * span), F32),
        pltpu.VMEM((depth, half), F32),
        pltpu.VMEM((depth, half), BF),
        pltpu.VMEM((chunks_of, parts - 1, sub, LANES), BF),
        pltpu.VMEM((others, chunks, frames) + inner + (depth,), BF),
        pltpu.SMEM((all_frames,), jnp.int32),
        pltpu.SMEM((frames,), jnp.int32),
        pltpu.VMEM((1, depth), F32),
        pltpu.VMEM((1, depth), F32),
        *arrivals, *sums,
        dma((2 * frames + 10 + (ranks - 1) * frames,)),
        dma((frames, chunks, others)), dma((frames, chunks, others)),
        dma((2, frames, ranks)), dma((2, frames, ranks)),
        dma((frames, chunks, others)), dma((frames, chunks, others)),
        dma((2, chunks, ranks)), dma((2, chunks, ranks)),
        dma((chunks,)), dma((chunks,)),
        dma((chunks, frames, others)), dma((chunks, frames, others)),
        dma((steps,)), dma((steps,)),
    ]
    by_columns = cotangent.reshape(frames, chunks, HALO, ranks, pc, depth)
    if inner[0] == 1:
        by_columns = by_columns.transpose(0, 1, 3, 2, 4, 5).reshape(frames, chunks, 1, ranks, blk, depth)
    out, grad = pl.pallas_call(
        functools.partial(block_kernel, dims),
        out_shape=(pltpu.VMEM((frames, chunks, inner[0], ranks, inner[1], depth), BF),
                   pltpu.VMEM((ny * sub, depth), F32)),
        in_specs=[anywhere] * 10,
        out_specs=(vmem, vmem),
        scratch_shapes=scratch,
        compiler_params=pltpu.CompilerParams(collective_id=0, has_side_effects=True,
                                             vmem_limit_bytes=60 << 20),
        name="block",
    )(clip_tokens.reshape(all_frames, chunks, blk, depth), frame_order.reshape(-1), row_reach.reshape(-1),
      spatial_gain.reshape(1, depth), temporal_gain.reshape(1, depth),
      spatial_heads, spatial_merge, temporal_heads, temporal_merge, by_columns)
    out, grad = pl.pallas_call(
        write_kernel,
        out_shape=(jax.ShapeDtypeStruct(out.shape, BF), jax.ShapeDtypeStruct(grad.shape, F32)),
        in_specs=[vmem, vmem],
        out_specs=(anywhere, anywhere),
        scratch_shapes=[dma((frames * chunks + 1,))],
        name="write",
    )(pltpu.with_memory_space_constraint(out, pltpu.VMEM), pltpu.with_memory_space_constraint(grad, pltpu.VMEM))
    if inner[0] == 1:
        out = out.reshape(frames, chunks, ranks, HALO, pc, depth).transpose(0, 1, 3, 2, 4, 5)
    return out.reshape(1, frames, rows, cols, depth), grad


def solution(mesh):
    in_specs = (
        P("batch", None, "space", "tm", None),
        P("batch", None),
        P("batch", "tm"),
        P(),
        P(),
        P(),
        P(),
        P(),
        P(),
        P("batch", "tm", "space", None, None),
    )
    out_specs = (P("batch", "tm", "space", None, None), P(("tm", "space"), None))
    return jax.shard_map(per_device, mesh=mesh, in_specs=in_specs, out_specs=out_specs, check_vma=False)
```
